8 devices in a mesh: t: 4 (over z, y, x), v: 2 (over core).
Axes of the slice: x: 2, y: 2, z: 1, core: 2. Of those that a mesh axis runs over, the one named last changes fastest.
Arguments:
- hidden_in: bfloat16 [1024, 2304], replicated
- seq_lens: int32 [1024], replicated
- target: int32 [1024], replicated
- g_attn_pre: bfloat16 [2304], replicated
- w_q: bfloat16 [2304, 2048], P(None, 't')
- w_k: bfloat16 [2304, 1024], P(None, 't')
- w_v: bfloat16 [2304, 1024], P(None, 't')
- w_o: bfloat16 [2048, 2304], P('t')
- g_attn_post: bfloat16 [2304], replicated
- g_mlp_pre: bfloat16 [2304], replicated
- w_gate: bfloat16 [2304, 9216], P(None, 't')
- w_up: bfloat16 [2304, 9216], P(None, 't')
- w_down: bfloat16 [9216, 2304], P('t')
- g_mlp_post: bfloat16 [2304], replicated
- g_final: bfloat16 [2304], replicated
- k_cache: bfloat16 [1024, 32, 4, 256], P(None, None, 't')
- v_cache: bfloat16 [1024, 32, 4, 256], P(None, None, 't')
- embed_table: bfloat16 [256000, 2304], P(('v', 't'))
Outputs:
- output 1: float32 [1024], replicated
- output 2: bfloat16 [1024, 2304], replicated
All inputs are finite; a program needn't handle non-finite values.
Results may differ from the reference program's by a relative error of at most 0.00791178.
Values sent between devices are 32-bit elements.
A program may use at most 1 GiB of HBM per device.

```python
import jax
import jax.numpy as jnp
from jax import lax

D = 2304
HEADS = 8
KV_HEADS = 4
HEAD = 256
FF = 9216
VOCAB = 256000
TOKENS = 1024
CTX = 32

ATTN_CAP = 50.0
FINAL_CAP = 30.0
NORM_EPS = 1e-6
ROPE_BASE = 10000.0


def rms_norm(values, gain_vec):
    x_f32 = values.astype(jnp.float32)
    scaled = x_f32 * lax.rsqrt(jnp.mean(x_f32 * x_f32, axis=-1, keepdims=True) + NORM_EPS)
    return scaled * (1.0 + gain_vec.astype(jnp.float32))


def rotary(values, positions):
    half_dim = values.shape[-1] // 2
    inv_freq = ROPE_BASE ** (-2.0 * jnp.arange(half_dim, dtype=jnp.float32) / values.shape[-1])
    angles = positions.astype(jnp.float32)[:, None] * inv_freq[None, :]
    angles = angles.reshape((values.shape[0],) + (1,) * (values.ndim - 2) + (half_dim,))
    cos_t = jnp.cos(angles)
    sin_t = jnp.sin(angles)
    x_low = values[..., :half_dim]
    x_high = values[..., half_dim:]
    return jnp.concatenate([x_low * cos_t - x_high * sin_t, x_high * cos_t + x_low * sin_t], axis=-1)


def setup_inputs(seed: int = 0) -> dict:
    keys = jax.random.split(jax.random.key(seed), 20)

    def normal_draw(sub_key, dims, scale_by):
        return (jax.random.normal(sub_key, dims, jnp.float32) * scale_by).astype(jnp.bfloat16)

    int_keys = jax.random.split(keys[19], 4)
    token_ids = jnp.arange(TOKENS)
    seq_lens = jax.random.randint(int_keys[0], (TOKENS,), 1, CTX + 1)
    picked = jax.random.permutation(int_keys[1], TOKENS)
    seq_lens = jnp.where(token_ids == picked[0], CTX, seq_lens)
    seq_lens = jnp.where(token_ids == picked[1], 1, seq_lens).astype(jnp.int32)
    stride = VOCAB // TOKENS
    target = token_ids * stride + jax.random.randint(int_keys[2], (TOKENS,), 0, stride)
    target = jax.random.permutation(int_keys[3], target).astype(jnp.int32)
    d_scale = D ** -0.5
    return {
        'hidden_in': normal_draw(keys[0], (TOKENS, D), 1.0),
        'seq_lens': seq_lens,
        'target': target,
        'g_attn_pre': normal_draw(keys[1], (D,), 0.4),
        'w_q': normal_draw(keys[2], (D, HEADS * HEAD), 4.0 * d_scale),
        'w_k': normal_draw(keys[3], (D, KV_HEADS * HEAD), 4.0 * d_scale),
        'w_v': normal_draw(keys[4], (D, KV_HEADS * HEAD), d_scale),
        'w_o': normal_draw(keys[5], (HEADS * HEAD, D), (HEADS * HEAD) ** -0.5),
        'g_attn_post': normal_draw(keys[6], (D,), 0.4),
        'g_mlp_pre': normal_draw(keys[7], (D,), 0.4),
        'w_gate': normal_draw(keys[8], (D, FF), d_scale),
        'w_up': normal_draw(keys[9], (D, FF), d_scale),
        'w_down': normal_draw(keys[10], (FF, D), FF ** -0.5),
        'g_mlp_post': normal_draw(keys[11], (D,), 0.4),
        'g_final': normal_draw(keys[12], (D,), 0.4),
        'k_cache': normal_draw(keys[13], (TOKENS, CTX, KV_HEADS, HEAD), 4.0),
        'v_cache': normal_draw(keys[14], (TOKENS, CTX, KV_HEADS, HEAD), 1.0),
        'embed_table': normal_draw(keys[15], (VOCAB, D), 25.0 * d_scale),
    }


def reference(hidden_in, seq_lens, target, g_attn_pre, w_q, w_k, w_v, w_o, g_attn_post, g_mlp_pre, w_gate, w_up, w_down, g_mlp_post, g_final, k_cache, v_cache, embed_table):
    group_size = HEADS // KV_HEADS
    score_scale = HEAD ** -0.5
    normed = rms_norm(hidden_in, g_attn_pre).astype(jnp.bfloat16)
    q_rot = rotary(jnp.dot(normed, w_q, preferred_element_type=jnp.float32).reshape(TOKENS, KV_HEADS, group_size, HEAD), seq_lens).astype(jnp.bfloat16)
    k_rot = rotary(jnp.dot(normed, w_k, preferred_element_type=jnp.float32).reshape(TOKENS, KV_HEADS, HEAD), seq_lens).astype(jnp.bfloat16)
    v_new = jnp.dot(normed, w_v, preferred_element_type=jnp.float32).astype(jnp.bfloat16).reshape(TOKENS, KV_HEADS, HEAD)

    def attend(operands):
        q_tok, k_tok, v_tok, keys_tok, vals_tok, len_tok = operands
        q_f32 = q_tok.astype(jnp.float32)
        s_cache = jnp.einsum('kgd,tkd->kgt', q_f32, keys_tok.astype(jnp.float32)) * score_scale
        s_new = jnp.einsum('kgd,kd->kg', q_f32, k_tok.astype(jnp.float32)) * score_scale
        s_cache = ATTN_CAP * jnp.tanh(s_cache / ATTN_CAP)
        s_new = ATTN_CAP * jnp.tanh(s_new / ATTN_CAP)
        s_cache = jnp.where(jnp.arange(CTX) < len_tok, s_cache, -1e30)
        row_max = jnp.maximum(jnp.max(s_cache, axis=-1), s_new)
        p_cache = jnp.exp(s_cache - row_max[..., None])
        p_new = jnp.exp(s_new - row_max)
        denominator = jnp.sum(p_cache, axis=-1) + p_new
        weighted = jnp.einsum('kgt,tkd->kgd', p_cache.astype(jnp.bfloat16).astype(jnp.float32), vals_tok.astype(jnp.float32))
        weighted = weighted + p_new.astype(jnp.bfloat16).astype(jnp.float32)[..., None] * v_tok.astype(jnp.float32)[:, None, :]
        return (weighted / denominator[..., None]).astype(jnp.bfloat16)

    attn_vec = lax.map(attend, (q_rot, k_rot, v_new, k_cache, v_cache, seq_lens))
    attn_out = jnp.dot(attn_vec.reshape(TOKENS, HEADS * HEAD), w_o, preferred_element_type=jnp.float32)
    hidden_mid = (hidden_in.astype(jnp.float32) + rms_norm(attn_out, g_attn_post)).astype(jnp.bfloat16)
    mlp_in = rms_norm(hidden_mid, g_mlp_pre).astype(jnp.bfloat16)
    gate_proj = jnp.dot(mlp_in, w_gate, preferred_element_type=jnp.float32)
    up_proj = jnp.dot(mlp_in, w_up, preferred_element_type=jnp.float32)
    activated = (jax.nn.gelu(gate_proj, approximate=True) * up_proj).astype(jnp.bfloat16)
    mlp_out = jnp.dot(activated, w_down, preferred_element_type=jnp.float32)
    hidden_out = (hidden_mid.astype(jnp.float32) + rms_norm(mlp_out, g_mlp_post)).astype(jnp.bfloat16)
    final_h = rms_norm(hidden_out, g_final).astype(jnp.bfloat16)

    blocks = 16
    block_rows = VOCAB // blocks
    table_blocks = embed_table.reshape(blocks, block_rows, D)
    starts = jnp.arange(blocks) * block_rows

    def block_stats(operands):
        table_block, start_row = operands
        logits = jnp.dot(final_h, table_block.T, preferred_element_type=jnp.float32)
        capped = FINAL_CAP * jnp.tanh(logits / FINAL_CAP)
        block_max = jnp.max(capped, axis=1)
        block_sum = jnp.sum(jnp.exp(capped - block_max[:, None]), axis=1)
        hit_mask = (start_row + jnp.arange(block_rows))[None, :] == target[:, None]
        block_tgt = jnp.sum(jnp.where(hit_mask, capped, 0.0), axis=1)
        return block_max, block_sum, block_tgt

    all_max, all_sum, all_tgt = lax.map(block_stats, (table_blocks, starts))
    glob_max = jnp.max(all_max, axis=0)
    log_norm = glob_max + jnp.log(jnp.sum(all_sum * jnp.exp(all_max - glob_max[None, :]), axis=0))
    logprob = jnp.sum(all_tgt, axis=0) - log_norm
    return logprob, hidden_out
```

```python
import jax
import jax.numpy as jnp
import numpy as np
from jax import lax
from jax.experimental import pallas as pl
from jax.experimental.pallas import tpu as pltpu
from jax.sharding import PartitionSpec as P

ATTN_CAP = 50.0
FINAL_CAP = 30.0
NORM_EPS = 1e-6
ROPE_BASE = 10000.0
LOG2E = 1.4426950408889634
BF16 = jnp.bfloat16
F32 = jnp.float32
VMEM_LIMIT = 60 * 1024 * 1024
VMEM_MAX = 67043328


def rms_norm(values, gain_vec):
    x_f32 = values.astype(F32)
    scaled = x_f32 * lax.rsqrt(jnp.mean(x_f32 * x_f32, axis=-1, keepdims=True) + NORM_EPS)
    return scaled * (1.0 + gain_vec.astype(F32))


def rope(vec, cos_t, sin_t):
    low, high = vec[:, :128], vec[:, 128:]
    out = jnp.concatenate([low * cos_t - high * sin_t, high * cos_t + low * sin_t], axis=1)
    return out.astype(BF16).astype(F32)


def attn_kernel(half_ref, x_ref, len_ref, g_ref, freq_ref, wq_ref, wk_ref, wv_ref, wo_ref, kc_ref, vc_ref, p_ref, o_scr):
    tb = x_ref.shape[0]
    groups = tb // 8
    scale = 1.0 / (16.0 * ATTN_CAP)
    a = rms_norm(x_ref[...], g_ref[0:1, :]).astype(BF16)
    q = jnp.dot(a, wq_ref[...], preferred_element_type=F32)
    k = jnp.dot(a, wk_ref[...], preferred_element_type=F32)
    v = jnp.dot(a, wv_ref[...], preferred_element_type=F32).astype(BF16).astype(F32)
    lens = jnp.broadcast_to(len_ref[0], (8, tb)).T[:, :1]
    ang = lens.astype(F32) * freq_ref[...]
    cos_t, sin_t = jnp.cos(ang), jnp.sin(ang)

    def pairs(first, second):
        both = jnp.stack([first.reshape(groups, 8, -1), second.reshape(groups, 8, -1)], axis=1)
        return both.reshape(2 * tb, first.shape[1])

    q_all = pairs(rope(q[:, :256], cos_t, sin_t), rope(q[:, 256:], cos_t, sin_t))
    k = rope(k, cos_t, sin_t)
    k_all, v_all, len_all = pairs(k, k), pairs(v, v), pairs(lens, lens)
    q_b = q_all.astype(BF16)
    nt = (((1,), (1,)), ((), ()))
    s = jnp.concatenate([lax.dot_general(q_b[16 * i:16 * i + 16], kc_ref[256 * i:256 * i + 256, :], nt, preferred_element_type=F32)
                         for i in range(groups)], axis=0)
    s = ATTN_CAP * jnp.tanh(s * scale)
    row = lax.broadcasted_iota(jnp.int32, s.shape, 0)
    col = lax.broadcasted_iota(jnp.int32, s.shape, 1)
    rel = col - (row % 8) * 32
    s = jnp.where((rel >= 0) & (rel < len_all), s, -1e30)
    s_new = ATTN_CAP * jnp.tanh(jnp.sum(q_all * k_all, axis=1, keepdims=True) * scale)
    top = jnp.maximum(jnp.max(s, axis=1, keepdims=True), s_new)
    e = jnp.exp(s - top)
    e_new = jnp.exp(s_new - top)
    den = jnp.sum(e, axis=1, keepdims=True) + e_new
    e_b = e.astype(BF16)
    o = jnp.concatenate([jnp.dot(e_b[16 * i:16 * i + 16], vc_ref[256 * i:256 * i + 256, :], preferred_element_type=F32)
                         for i in range(groups)], axis=0)
    o = (o + e_new.astype(BF16).astype(F32) * v_all) / den
    for i in range(groups):
        o_scr[8 * i:8 * i + 8, :256] = o[16 * i:16 * i + 8]
        o_scr[8 * i:8 * i + 8, 256:] = o[16 * i + 8:16 * i + 16]
    o_b = o_scr[...].astype(BF16)
    mid = wo_ref.shape[1] // 2
    p_ref[0] = jnp.dot(o_b, wo_ref[:, :mid], preferred_element_type=F32)
    p_ref[1] = jnp.dot(o_b, wo_ref[:, mid:], preferred_element_type=F32)


def attention(half, x, lens, g, freq, wq, wk, wv, wo, kc, vc, tb=128):
    n = x.shape[0] // 2
    nb = n // tb
    d = x.shape[1]
    full = lambda s: pl.BlockSpec(s, lambda i, h: (0, 0))
    rows = lambda r, c: pl.BlockSpec((r, c), lambda i, h: (h[0] * nb + i, 0))
    return pl.pallas_call(
        attn_kernel,
        grid_spec=pltpu.PrefetchScalarGridSpec(
            num_scalar_prefetch=1, grid=(nb,),
            in_specs=[rows(tb, d), pl.BlockSpec((1, 1, tb), lambda i, h: (h[0] * nb + i, 0, 0)), full(g.shape), full(freq.shape), full(wq.shape), full(wk.shape),
                      full(wv.shape), full(wo.shape), rows(tb * 32, 256), rows(tb * 32, 256)],
            out_specs=pl.BlockSpec((2, tb, d // 2), lambda i, h: (0, i, 0)),
            scratch_shapes=[pltpu.VMEM((tb, 512), F32)]),
        out_shape=jax.ShapeDtypeStruct((2, n, d // 2), F32),
        compiler_params=pltpu.CompilerParams(vmem_limit_bytes=VMEM_LIMIT),
        name='attn',
    )(half, x, lens, g, freq, wq, wk, wv, wo, kc, vc)


MESH = pl.DeviceIdType.MESH
CHUNKS = 4
OWN = 128
PART = OWN // CHUNKS
COLS = 1152


def place():
    t, v = lax.axis_index('t'), lax.axis_index('v')
    return t, v, t + 1 - 2 * (t % 2), (t + 2) % 4, 3 - t


def meet_all(t, v):
    barrier = pltpu.get_barrier_semaphore()
    for dt in range(4):
        for dv in range(2):
            if dt or dv:
                pl.semaphore_signal(barrier, inc=1, device_id=((t + dt) % 4, (v + dv) % 2), device_id_type=MESH)
    pl.semaphore_wait(barrier, 7)


def send(src, dst, sems, idx, dev):
    return pltpu.make_async_remote_copy(src_ref=src, dst_ref=dst, send_sem=sems.at[(0,) + idx], recv_sem=sems.at[(1,) + idx],
                                        device_id=dev, device_id_type=MESH)


def norm_halves(h0, h1, g_ref):
    d = 2 * h0.shape[1]
    inv = lax.rsqrt((jnp.sum(h0 * h0, axis=1, keepdims=True) + jnp.sum(h1 * h1, axis=1, keepdims=True)) / d + NORM_EPS)
    return h0 * inv * (1.0 + g_ref[:, :COLS]), h1 * inv * (1.0 + g_ref[:, COLS:])


def layer_kernel(p1, x_hbm, gains, wg_hbm, wu_hbm, wd_hbm, y_ref,
                 wg, wu, wd, xb, x1, r1, r2, r3, r4, fwd, ag, p2, mb, act, loads, s1, s2, s3, s4, s5, s6):
    t, v, tx, ty, tz = place()
    dev_x, dev_y = (tx, v), (ty, v)
    g_post, g_pre, g_mlp = gains[1:2, :], gains[2:3, :], gains[3:4, :]
    rows = lambda q, c: pl.ds(pl.multiple_of(q * OWN + c * PART, PART), PART)
    part = lambda c: pl.ds(pl.multiple_of(c * PART, PART), PART)
    weights = [pltpu.make_async_copy(a, b, loads.at[i]) for i, (a, b) in enumerate(((wg_hbm, wg), (wu_hbm, wu), (wd_hbm, wd)))]
    x_load = pltpu.make_async_copy(x_hbm.at[pl.ds(pl.multiple_of((v * 4 + t) * OWN, OWN), OWN)], xb, loads.at[3])
    x_load.start()
    for w in weights:
        w.start()
    meet_all(t, v)

    def rs_first(p, r, sems, c):
        return [send(p.at[h, rows(q, c)], r.at[h, slot, part(c)], sems, (c, 2 * h + slot), dev)
                for h, slot, q, dev in ((0, 1, tz, dev_x), (1, 1, tz, dev_y), (0, 0, tx, dev_x), (1, 0, ty, dev_y))]

    def rs_second(r, sems, c):
        return [send(fwd.at[h, part(c)], r.at[h, part(c)], sems, (c, h), dev) for h, dev in ((0, dev_y), (1, dev_x))]

    def rs_forward(p, r, r_next, sems, sems_next, c):
        first = rs_first(p, r, sems, c)
        for h, q, cp in ((0, ty, rs_second(r_next, sems_next, c)[0]), (1, tx, rs_second(r_next, sems_next, c)[1])):
            first[h].wait_recv()
            fwd[h, part(c)] = p[h, rows(q, c)] + r[h, 1, part(c)]
            cp.start()

    def rs_finish(p, r, r_next, sems, sems_next, c):
        first, second = rs_first(p, r, sems, c), rs_second(r_next, sems_next, c)
        out = []
        for h in range(2):
            first[2 + h].wait_recv()
            second[h].wait_recv()
            out.append(p[h, rows(t, c)] + r[h, 0, part(c)] + r_next[h, part(c)])
        for cp in first + second:
            cp.wait_send()
        return out

    def ag_first(c):
        return [send(ag.at[h, rows(t, c)], ag.at[h, rows(t, c)], s3, (c, i), dev)
                for i, (h, dev) in enumerate(((0, dev_x), (1, dev_y), (1, dev_x), (0, dev_y)))]

    def ag_second(c):
        return [send(ag.at[h, rows(q, c)], ag.at[h, rows(q, c)], s4, (c, h), dev) for h, q, dev in ((0, tx, dev_y), (1, ty, dev_x))]

    def each(body):
        lax.fori_loop(0, CHUNKS, lambda c, _: (body(c), 0)[1], 0)

    @each
    def _(c):
        for cp in rs_first(p1, r1, s1, c):
            cp.start()

    @each
    def _(c):
        rs_forward(p1, r1, r2, s1, s2, c)

    x_load.wait()

    @each
    def _(c):
        s_a, s_b = norm_halves(*rs_finish(p1, r1, r2, s1, s2, c), g_post)
        x_a = (xb[part(c), :COLS].astype(F32) + s_a).astype(BF16)
        x_b = (xb[part(c), COLS:].astype(F32) + s_b).astype(BF16)
        x1[part(c), :COLS] = x_a
        x1[part(c), COLS:] = x_b
        m_a, m_b = norm_halves(x_a.astype(F32), x_b.astype(F32), g_pre)
        ag[0, rows(t, c)] = m_a.astype(BF16).astype(F32)
        ag[1, rows(t, c)] = m_b.astype(BF16).astype(F32)
        for cp in ag_first(c):
            cp.start()

    @each
    def _(c):
        for cp, nxt in zip(ag_first(c)[:2], ag_second(c)):
            cp.wait_recv()
            nxt.start()

    for w in weights:
        w.wait()

    @each
    def _(c):
        for cp in ag_first(c)[2:] + ag_second(c):
            cp.wait_recv()
        for q in range(4):
            for h in range(2):
                mb[PART * q:PART * q + PART, COLS * h:COLS * h + COLS] = ag[h, rows(q, c)].astype(BF16)

        def up(j, _):
            cols = pl.ds(pl.multiple_of(j * 256, 256), 256)
            gate = jnp.dot(mb[...], wg[:, cols], preferred_element_type=F32)
            lift = jnp.dot(mb[...], wu[:, cols], preferred_element_type=F32)
            act[:, cols] = (jax.nn.gelu(gate, approximate=True) * lift).astype(BF16)
            return 0

        lax.fori_loop(0, wg.shape[1] // 256, up, 0)
        for h in range(2):
            def down(j, _):
                res = jnp.dot(act[...], wd[:, pl.ds(pl.multiple_of(COLS * h + j * 384, 128), 384)], preferred_element_type=F32)
                for q in range(4):
                    p2[h, rows(q, c), pl.ds(pl.multiple_of(j * 384, 128), 384)] = res[PART * q:PART * q + PART]
                return 0

            lax.fori_loop(0, COLS // 384, down, 0)
        for cp in rs_first(p2, r3, s5, c):
            cp.start()

    @each
    def _(c):
        rs_forward(p2, r3, r4, s5, s6, c)

    @each
    def _(c):
        s_a, s_b = norm_halves(*rs_finish(p2, r3, r4, s5, s6, c), g_mlp)
        y_ref[0, part(c)] = (x1[part(c), :COLS].astype(F32) + s_a).astype(BF16).astype(F32)
        y_ref[1, part(c)] = (x1[part(c), COLS:].astype(F32) + s_b).astype(BF16).astype(F32)
        for cp in ag_first(c) + ag_second(c):
            cp.wait_send()


def layer(p1, x, gains, wg, wu, wd):
    d, f = wg.shape
    n = p1.shape[1]
    vm, hbm = pl.BlockSpec(memory_space=pltpu.VMEM), pl.BlockSpec(memory_space=pl.ANY)
    sem = lambda k: pltpu.SemaphoreType.DMA((2, CHUNKS, k))
    return pl.pallas_call(
        layer_kernel,
        out_shape=jax.ShapeDtypeStruct((2, OWN, COLS), F32),
        in_specs=[vm, hbm, vm, hbm, hbm, hbm],
        out_specs=vm,
        scratch_shapes=[
            pltpu.VMEM((d, f), BF16), pltpu.VMEM((d, f), BF16), pltpu.VMEM((f, d), BF16),
            pltpu.VMEM((OWN, d), BF16), pltpu.VMEM((OWN, d), BF16),
            pltpu.VMEM((2, 2, OWN, COLS), F32), pltpu.VMEM((2, OWN, COLS), F32),
            pltpu.VMEM((2, 2, OWN, COLS), F32), pltpu.VMEM((2, OWN, COLS), F32),
            pltpu.VMEM((2, OWN, COLS), F32), pltpu.VMEM((2, n, COLS), F32), pltpu.VMEM((2, n, COLS), F32),
            pltpu.VMEM((OWN, d), BF16), pltpu.VMEM((OWN, f), BF16),
            pltpu.SemaphoreType.DMA((4,)), sem(4), sem(2), sem(4), sem(2), sem(4), sem(2)],
        compiler_params=pltpu.CompilerParams(collective_id=0, has_side_effects=True, vmem_limit_bytes=VMEM_MAX),
        name='layer',
    )(p1, x, gains, wg, wu, wd)


TILE = 640
SLOTS = 3


def head_epilogue(logits, diff, base):
    tv, n = logits.shape
    th = jnp.tanh(logits * (1.0 / FINAL_CAP)).reshape(tv // 8, 8, n)
    ex = jnp.exp2(th * (FINAL_CAP * LOG2E))
    rows = lax.broadcasted_iota(jnp.int32, th.shape, 0) * 8
    hit = jnp.where((diff - base)[None] == rows, th, 0.0)
    return jnp.sum(ex, axis=0), jnp.sum(hit, axis=0)


def head_kernel(y_own, gains, tgt, e_hbm, y_out, lp_ref,
                ag, yb, ht, eb, lg_a, lg_b, dif, tot, hit, part, fin, e_sem, y_sem, s1, s2, s3, s4):
    t, v, tx, ty, tz = place()
    me = v * 4 + t
    dev_x, dev_y, dev_p = (tx, v), (ty, v), (t, 1 - v)
    chips = (t, tx, ty, tz)
    g_fin = gains[4:5, :]
    vocab = e_hbm.shape[0]
    pairs = vocab // (2 * TILE)
    total = 2 * pairs

    def fetch(g):
        src = e_hbm.at[pl.ds(pl.multiple_of((g % pairs) * (2 * TILE), 2 * TILE), 2 * TILE)]
        return pltpu.make_async_copy(src, eb.at[g % SLOTS], e_sem.at[g % SLOTS])

    for g in range(SLOTS - 1):
        fetch(g).start()
    meet_all(t, v)

    first = [send(y_own.at[h], ag.at[h, me], s1, (i,), dev)
             for i, (h, dev) in enumerate(((0, dev_x), (1, dev_y), (1, dev_x), (0, dev_y)))]
    second = [send(ag.at[h, v * 4 + q], ag.at[h, v * 4 + q], s2, (h,), dev) for h, q, dev in ((0, tx, dev_y), (1, ty, dev_x))]
    cross = [send(y_own, ag.at[:, me], s3, (0,), dev_p)]
    cross += [send(ag.at[:, v * 4 + q], ag.at[:, v * 4 + q], s3, (i + 1,), dev_p) for i, q in enumerate((tx, ty, tz))]
    cross[0].start()
    for cp in first:
        cp.start()
    tot[...] = jnp.zeros_like(tot)
    hit[...] = jnp.zeros_like(hit)
    for g, q in enumerate(chips):
        for w in range(2):
            lane = tgt[w * 4 + q] - me * vocab
            dif[g, :, 128 * w:128 * w + 128] = lane - lax.broadcasted_iota(jnp.int32, (8, 128), 0)

    def y_copy(b):
        return pltpu.make_async_copy(yb.at[b], y_out.at[pl.ds(pl.multiple_of(b * OWN, OWN), OWN)], y_sem.at[b])

    def prepare(src, b, g, w):
        h_a, h_b = src(0), src(1)
        yb[b, :, :COLS] = h_a.astype(BF16)
        yb[b, :, COLS:] = h_b.astype(BF16)
        y_copy(b).start()
        n_a, n_b = norm_halves(h_a, h_b, g_fin)
        ht[g, :COLS, 128 * w:128 * w + 128] = n_a.T.astype(BF16)
        ht[g, COLS:, 128 * w:128 * w + 128] = n_b.T.astype(BF16)

    def prepare_chip(g, q):
        for w in range(2):
            prepare(lambda h: ag[h, w * 4 + q], w * 4 + q, g, w)

    def mine(h):
        return y_own[h]

    cross[0].wait_recv()
    for w in range(2):
        @pl.when(v == w)
        def _():
            prepare(mine, me, 0, w)
            prepare(lambda h: ag[h, (1 - w) * 4 + t], (1 - w) * 4 + t, 0, 1 - w)

    def epilogue(lg, g, base, valid):
        s, k = head_epilogue(lg[...], dif[g], base)
        tot[g] += jnp.where(valid, s, 0.0)
        hit[g] += jnp.where(valid, k, 0.0)

    def body(i, offset, groups):
        g = i + offset
        slot = g % SLOTS
        fetch(g).wait()

        @pl.when(g + SLOTS - 1 < total)
        def _():
            fetch(g + SLOTS - 1).start()

        last = (groups[-1], (2 * i - 1) * TILE, i > 0)
        bufs = (lg_a, lg_b)
        count = 0
        for k in range(2):
            for grp in groups:
                cur, prev = bufs[count % 2], bufs[(count + 1) % 2]
                cur[...] = jnp.dot(eb[slot, TILE * k:TILE * k + TILE, :], ht[grp], preferred_element_type=F32)
                epilogue(prev, *last)
                last = (grp, (2 * i + k) * TILE, True)
                count += 1

    def pass_one(i, _):
        @pl.when(i == 9)
        def _():
            for cp, nxt in zip(first[:2], second):
                cp.wait_recv()
                nxt.start()

        @pl.when(i == 18)
        def _():
            for cp in first[2:]:
                cp.wait_recv()
            cross[1].start()
            cross[2].start()

        body(i, 0, (0,))
        return 0

    lax.fori_loop(0, pairs, pass_one, 0)
    epilogue(lg_b, 0, (2 * pairs - 1) * TILE, True)
    for cp in second:
        cp.wait_recv()
    cross[3].start()
    for g in (1, 2, 3):
        cross[g].wait_recv()
        prepare_chip(g, chips[g])
    lax.fori_loop(0, pairs, lambda i, _: (body(i, pairs, (1, 2, 3)), 0)[1], 0)
    epilogue(lg_b, 3, (2 * pairs - 1) * TILE, True)

    for g, q in enumerate(chips):
        for w in range(2):
            lanes = slice(128 * w, 128 * w + 128)
            part[w * 4 + q, 0:1] = jnp.sum(tot[g, :, lanes], axis=0, keepdims=True)
            part[w * 4 + q, 1:2] = jnp.sum(hit[g, :, lanes], axis=0, keepdims=True)
    outs = []
    for k in range(1, 8):
        dt, dv = k % 4, k // 4
        outs.append(send(part, fin.at[k], s4, (k - 1,), ((t + dt) % 4, (v + dv) % 2)))
    for cp in outs:
        cp.start()
    acc = part[...]
    for k in range(1, 8):
        outs[k - 1].wait_recv()
        acc += fin[k]
    lp_ref[...] = FINAL_CAP * acc[:, 1] - jnp.log(acc[:, 0])
    for cp in first + second + cross + outs:
        cp.wait_send()
    for b in range(8):
        y_copy(b).wait()


def head(y_own, gains, tgt, table):
    d = table.shape[1]
    vm, hbm = pl.BlockSpec(memory_space=pltpu.VMEM), pl.BlockSpec(memory_space=pl.ANY)
    return pl.pallas_call(
        head_kernel,
        out_shape=[jax.ShapeDtypeStruct((8 * OWN, d), BF16), jax.ShapeDtypeStruct((8, OWN), F32)],
        in_specs=[vm, vm, vm, hbm],
        out_specs=[hbm, vm],
        scratch_shapes=[
            pltpu.VMEM((2, 8, OWN, COLS), F32), pltpu.VMEM((8, OWN, d), BF16), pltpu.VMEM((4, d, 256), BF16),
            pltpu.VMEM((SLOTS, 2 * TILE, d), BF16), pltpu.VMEM((TILE, 256), F32), pltpu.VMEM((TILE, 256), F32),
            pltpu.VMEM((4, 8, 256), jnp.int32), pltpu.VMEM((4, 8, 256), F32), pltpu.VMEM((4, 8, 256), F32),
            pltpu.VMEM((8, 2, OWN), F32), pltpu.VMEM((8, 8, 2, OWN), F32),
            pltpu.SemaphoreType.DMA((SLOTS,)), pltpu.SemaphoreType.DMA((8,)),
            pltpu.SemaphoreType.DMA((2, 4)), pltpu.SemaphoreType.DMA((2, 2)), pltpu.SemaphoreType.DMA((2, 4)), pltpu.SemaphoreType.DMA((2, 7))],
        compiler_params=pltpu.CompilerParams(collective_id=1, has_side_effects=True, vmem_limit_bytes=VMEM_MAX),
        name='head',
    )(y_own, gains, tgt, table)


def solution(mesh):
    in_specs = (P(), P(), P(), P(), P(None, 't'), P(None, 't'), P(None, 't'), P('t', None), P(), P(), P(None, 't'), P(None, 't'), P('t', None), P(), P(), P(None, None, 't', None), P(None, None, 't', None), P(('v', 't'), None))

    def local_step(hidden_in, seq_lens, target, g_attn_pre, w_q, w_k, w_v, w_o, g_attn_post, g_mlp_pre, w_gate, w_up, w_down, g_mlp_post, g_final, k_cache, v_cache, embed_table):
        half = lax.axis_index('v')
        gains = jnp.stack([g_attn_pre, g_attn_post, g_mlp_pre, g_mlp_post, g_final]).astype(F32)
        freq = jnp.asarray((ROPE_BASE ** (-2.0 * np.arange(128, dtype=np.float32) / 256)).astype(np.float32)[None])
        p1 = attention(half[None].astype(jnp.int32), hidden_in, seq_lens.reshape(-1, 1, 128), gains, freq, w_q, w_k, w_v, w_o,
                       k_cache.reshape(-1, 256), v_cache.reshape(-1, 256))
        y_own = layer(p1, hidden_in, gains, w_gate, w_up, w_down)
        hidden_out, logprob = head(y_own, gains, target.reshape(8, 1, OWN), embed_table)
        return logprob.reshape(-1), hidden_out

    return jax.shard_map(local_step, mesh=mesh, in_specs=in_specs, out_specs=(P(), P()), check_vma=False)
```

```python
import jax
import jax.numpy as jnp
import numpy as np
from jax import lax
from jax.experimental import pallas as pl
from jax.experimental.pallas import tpu as pltpu
from jax.sharding import PartitionSpec as P

ATTN_CAP = 50.0
FINAL_CAP = 30.0
NORM_EPS = 1e-6
ROPE_BASE = 10000.0
LOG2E = 1.4426950408889634
BF16 = jnp.bfloat16
F32 = jnp.float32
VMEM_LIMIT = 60 * 1024 * 1024
VMEM_MAX = 67043328


def rms_norm(values, gain_vec):
    x_f32 = values.astype(F32)
    scaled = x_f32 * lax.rsqrt(jnp.mean(x_f32 * x_f32, axis=-1, keepdims=True) + NORM_EPS)
    return scaled * (1.0 + gain_vec.astype(F32))


def rope(vec, cos_t, sin_t):
    low, high = vec[:, :128], vec[:, 128:]
    out = jnp.concatenate([low * cos_t - high * sin_t, high * cos_t + low * sin_t], axis=1)
    return out.astype(BF16).astype(F32)


def attend(x, lens, gain, freq, wq, wk, wv, wo, keys, vals, put):
    tb = x.shape[0]
    groups = tb // 8
    scale = 1.0 / (16.0 * ATTN_CAP)
    a = rms_norm(x, gain).astype(BF16)
    q = jnp.dot(a, wq, preferred_element_type=F32)
    k = jnp.dot(a, wk, preferred_element_type=F32)
    v = jnp.dot(a, wv, preferred_element_type=F32).astype(BF16).astype(F32)
    ang = lens.astype(F32) * freq
    cos_t, sin_t = jnp.cos(ang), jnp.sin(ang)

    def pairs(first, second):
        both = jnp.stack([first.reshape(groups, 8, -1), second.reshape(groups, 8, -1)], axis=1)
        return both.reshape(2 * tb, first.shape[1])

    q_all = pairs(rope(q[:, :256], cos_t, sin_t), rope(q[:, 256:], cos_t, sin_t))
    k = rope(k, cos_t, sin_t)
    k_all, v_all, len_all = pairs(k, k), pairs(v, v), pairs(lens, lens)
    q_b = q_all.astype(BF16)
    nt = (((1,), (1,)), ((), ()))
    s = jnp.concatenate([lax.dot_general(q_b[16 * i:16 * i + 16], keys(i), nt, preferred_element_type=F32)
                         for i in range(groups)], axis=0)
    s = ATTN_CAP * jnp.tanh(s * scale)
    row = lax.broadcasted_iota(jnp.int32, s.shape, 0)
    col = lax.broadcasted_iota(jnp.int32, s.shape, 1)
    rel = col - (row % 8) * 32
    s = jnp.where((rel >= 0) & (rel < len_all), s, -1e30)
    s_new = ATTN_CAP * jnp.tanh(jnp.sum(q_all * k_all, axis=1, keepdims=True) * scale)
    top = jnp.maximum(jnp.max(s, axis=1, keepdims=True), s_new)
    e = jnp.exp(s - top)
    e_new = jnp.exp(s_new - top)
    den = jnp.sum(e, axis=1, keepdims=True) + e_new
    e_b = e.astype(BF16)
    o = jnp.concatenate([jnp.dot(e_b[16 * i:16 * i + 16], vals(i), preferred_element_type=F32) for i in range(groups)], axis=0)
    o = ((o + e_new.astype(BF16).astype(F32) * v_all) / den).reshape(groups, 2, 8, 256)
    o_b = jnp.concatenate([o[:, 0].reshape(tb, 256), o[:, 1].reshape(tb, 256)], axis=1).astype(BF16)
    for j in range(wo.shape[1] // 384):
        put(j, jnp.dot(o_b, wo[:, 384 * j:384 * j + 384], preferred_element_type=F32))


MESH = pl.DeviceIdType.MESH
CHUNKS = 4
OWN = 128
PART = OWN // CHUNKS
COLS = 1152


def place():
    t, v = lax.axis_index('t'), lax.axis_index('v')
    return t, v, t + 1 - 2 * (t % 2), (t + 2) % 4, 3 - t


def meet_all(t, v):
    barrier = pltpu.get_barrier_semaphore()
    for dt in range(4):
        for dv in range(2):
            if dt or dv:
                pl.semaphore_signal(barrier, inc=1, device_id=((t + dt) % 4, (v + dv) % 2), device_id_type=MESH)
    pl.semaphore_wait(barrier, 7)


def send(src, dst, sems, idx, dev):
    return pltpu.make_async_remote_copy(src_ref=src, dst_ref=dst, send_sem=sems.at[(0,) + idx], recv_sem=sems.at[(1,) + idx],
                                        device_id=dev, device_id_type=MESH)


def norm_halves(h0, h1, g_ref):
    d = 2 * h0.shape[1]
    inv = lax.rsqrt((jnp.sum(h0 * h0, axis=1, keepdims=True) + jnp.sum(h1 * h1, axis=1, keepdims=True)) / d + NORM_EPS)
    return h0 * inv * (1.0 + g_ref[:, :COLS]), h1 * inv * (1.0 + g_ref[:, COLS:])


def layer_kernel(x_hbm, lens, gains, freq, wq_hbm, wk_hbm, wv_hbm, wo_hbm, kc_hbm, vc_hbm, wg_hbm, wu_hbm, wd_hbm, y_ref,
                 bank, xh, x1, p1, r1, r2, r3, r4, fwd, ag, p2, mb, act, lens_s, loads, caches, s1, s2, s3, s4, s5, s6):
    t, v, tx, ty, tz = place()
    dev_x, dev_y = (tx, v), (ty, v)
    g_post, g_pre, g_mlp = gains[1:2, :], gains[2:3, :], gains[3:4, :]
    d = xh.shape[1]
    rows = lambda q, c: pl.ds(pl.multiple_of(q * OWN + c * PART, PART), PART)
    part = lambda c: pl.ds(pl.multiple_of(c * PART, PART), PART)
    wq, wk, wv, wo = bank.at[:d, :512], bank.at[:d, 512:768], bank.at[:d, 768:1024], bank.at[d:d + 512]
    cache_row = d + 512
    wg, wu, wd = bank.at[:d], bank.at[d:2 * d], bank.at[2 * d:]
    local = pltpu.make_async_copy
    early = [local(a, b, loads.at[i]) for i, (a, b) in enumerate((
        (x_hbm.at[pl.ds(pl.multiple_of(v * 4 * OWN, 4 * OWN), 4 * OWN)], xh), (wq_hbm, wq), (wk_hbm, wk), (wv_hbm, wv)))]
    wo_load = local(wo_hbm, wo, loads.at[4])
    weights = [local(a, b, loads.at[5 + i]) for i, (a, b) in enumerate(((wg_hbm, wg), (wu_hbm, wu), (wd_hbm, wd)))]

    def cache_load(c):
        out = []
        for i, src in enumerate((kc_hbm, vc_hbm)):
            for q in range(4):
                first = pl.multiple_of(((v * 4 + q) * OWN + c * PART) * 32, PART * 32)
                out.append(local(src.at[pl.ds(first, PART * 32)],
                                 bank.at[pl.ds(cache_row + q * PART * 32, PART * 32), pl.ds(pl.multiple_of((2 * c + i) * 256, 256), 256)],
                                 caches.at[c, 4 * i + q]))
        return out

    for cp in early:
        cp.start()
    for cp in cache_load(0):
        cp.start()
    wo_load.start()
    for c in range(1, CHUNKS):
        for cp in cache_load(c):
            cp.start()
    for q in range(4):
        lens_s[OWN * q:OWN * q + OWN, :] = jnp.broadcast_to(lens[v * 4 + q], (OWN, OWN)).T
    meet_all(t, v)
    for cp in early:
        cp.wait()

    def rs_first(p, r, sems, c):
        return [send(p.at[h, rows(q, c)], r.at[h, slot, part(c)], sems, (c, 2 * h + slot), dev)
                for h, slot, q, dev in ((0, 1, tz, dev_x), (1, 1, tz, dev_y), (0, 0, tx, dev_x), (1, 0, ty, dev_y))]

    def rs_second(r, sems, c):
        return [send(fwd.at[h, part(c)], r.at[h, part(c)], sems, (c, h), dev) for h, dev in ((0, dev_y), (1, dev_x))]

    def rs_forward(p, r, r_next, sems, sems_next, c):
        first = rs_first(p, r, sems, c)
        for h, q, cp in ((0, ty, rs_second(r_next, sems_next, c)[0]), (1, tx, rs_second(r_next, sems_next, c)[1])):
            first[h].wait_recv()
            fwd[h, part(c)] = p[h, rows(q, c)] + r[h, 1, part(c)]
            cp.start()

    def rs_finish(p, r, r_next, sems, sems_next, c):
        first, second = rs_first(p, r, sems, c), rs_second(r_next, sems_next, c)
        out = []
        for h in range(2):
            first[2 + h].wait_recv()
            second[h].wait_recv()
            out.append(p[h, rows(t, c)] + r[h, 0, part(c)] + r_next[h, part(c)])
        for cp in first + second:
            cp.wait_send()
        return out

    def ag_first(c):
        return [send(ag.at[h, rows(t, c)], ag.at[h, rows(t, c)], s3, (c, i), dev)
                for i, (h, dev) in enumerate(((0, dev_x), (1, dev_y), (1, dev_x), (0, dev_y)))]

    def ag_second(c):
        return [send(ag.at[h, rows(q, c)], ag.at[h, rows(q, c)], s4, (c, h), dev) for h, q, dev in ((0, tx, dev_y), (1, ty, dev_x))]

    def each(body):
        lax.fori_loop(0, CHUNKS, lambda c, _: (body(c), 0)[1], 0)

    @each
    def _(c):
        for cp in cache_load(c):
            cp.wait()

        @pl.when(c == 0)
        def _():
            wo_load.wait()

        x = jnp.concatenate([xh[rows(q, c), :] for q in range(4)], axis=0)
        lens_c = jnp.concatenate([lens_s[rows(q, c), :1] for q in range(4)], axis=0)

        def cached(i):
            return lambda g: bank[pl.ds(cache_row + 256 * g, 256), pl.ds(pl.multiple_of((2 * c + i) * 256, 256), 256)]

        def put(j, res):
            h, first = j // 3, 384 * (j % 3)
            for q in range(4):
                p1[h, rows(q, c), first:first + 384] = res[PART * q:PART * q + PART]

        attend(x, lens_c, gains[0:1, :], freq[...], wq[...], wk[...], wv[...], wo, cached(0), cached(1), put)
        for cp in rs_first(p1, r1, s1, c):
            cp.start()

    for w in weights:
        w.start()

    @each
    def _(c):
        rs_forward(p1, r1, r2, s1, s2, c)

    @each
    def _(c):
        s_a, s_b = norm_halves(*rs_finish(p1, r1, r2, s1, s2, c), g_post)
        x_a = (xh[rows(t, c), :COLS].astype(F32) + s_a).astype(BF16)
        x_b = (xh[rows(t, c), COLS:].astype(F32) + s_b).astype(BF16)
        x1[part(c), :COLS] = x_a
        x1[part(c), COLS:] = x_b
        m_a, m_b = norm_halves(x_a.astype(F32), x_b.astype(F32), g_pre)
        ag[0, rows(t, c)] = m_a.astype(BF16).astype(F32)
        ag[1, rows(t, c)] = m_b.astype(BF16).astype(F32)
        for cp in ag_first(c):
            cp.start()

    @each
    def _(c):
        for cp, nxt in zip(ag_first(c)[:2], ag_second(c)):
            cp.wait_recv()
            nxt.start()

    for w in weights:
        w.wait()

    @each
    def _(c):
        for cp in ag_first(c)[2:] + ag_second(c):
            cp.wait_recv()
        for q in range(4):
            for h in range(2):
                mb[PART * q:PART * q + PART, COLS * h:COLS * h + COLS] = ag[h, rows(q, c)].astype(BF16)

        def up(j, _):
            cols = pl.ds(pl.multiple_of(j * 256, 256), 256)
            gate = jnp.dot(mb[...], wg[:, cols], preferred_element_type=F32)
            lift = jnp.dot(mb[...], wu[:, cols], preferred_element_type=F32)
            act[:, cols] = (jax.nn.gelu(gate, approximate=True) * lift).astype(BF16)
            return 0

        lax.fori_loop(0, d // 256, up, 0)
        for h in range(2):
            def down(j, _):
                res = jnp.dot(act[...], wd[:, pl.ds(pl.multiple_of(COLS * h + j * 384, 128), 384)], preferred_element_type=F32)
                for q in range(4):
                    p2[h, rows(q, c), pl.ds(pl.multiple_of(j * 384, 128), 384)] = res[PART * q:PART * q + PART]
                return 0

            lax.fori_loop(0, COLS // 384, down, 0)
        for cp in rs_first(p2, r3, s5, c):
            cp.start()

    @each
    def _(c):
        rs_forward(p2, r3, r4, s5, s6, c)

    @each
    def _(c):
        s_a, s_b = norm_halves(*rs_finish(p2, r3, r4, s5, s6, c), g_mlp)
        y_ref[0, part(c)] = (x1[part(c), :COLS].astype(F32) + s_a).astype(BF16).astype(F32)
        y_ref[1, part(c)] = (x1[part(c), COLS:].astype(F32) + s_b).astype(BF16).astype(F32)
        for cp in ag_first(c) + ag_second(c):
            cp.wait_send()


def layer(x, lens, gains, freq, wq, wk, wv, wo, kc, vc, wg, wu, wd):
    d = x.shape[1]
    n = x.shape[0] // 2
    vm, hbm = pl.BlockSpec(memory_space=pltpu.VMEM), pl.BlockSpec(memory_space=pl.ANY)
    sem = lambda k: pltpu.SemaphoreType.DMA((2, CHUNKS, k))
    return pl.pallas_call(
        layer_kernel,
        out_shape=jax.ShapeDtypeStruct((2, OWN, COLS), F32),
        in_specs=[hbm, vm, vm, vm] + [hbm] * 9,
        out_specs=vm,
        scratch_shapes=[
            pltpu.VMEM((3 * d, d), BF16), pltpu.VMEM((n, d), BF16), pltpu.VMEM((OWN, d), BF16), pltpu.VMEM((2, n, COLS), F32),
            pltpu.VMEM((2, 2, OWN, COLS), F32), pltpu.VMEM((2, OWN, COLS), F32),
            pltpu.VMEM((2, 2, OWN, COLS), F32), pltpu.VMEM((2, OWN, COLS), F32),
            pltpu.VMEM((2, OWN, COLS), F32), pltpu.VMEM((2, n, COLS), F32), pltpu.VMEM((2, n, COLS), F32),
            pltpu.VMEM((OWN, d), BF16), pltpu.VMEM((OWN, d), BF16), pltpu.VMEM((n, 128), jnp.int32),
            pltpu.SemaphoreType.DMA((8,)), pltpu.SemaphoreType.DMA((CHUNKS, 8)),
            sem(4), sem(2), sem(4), sem(2), sem(4), sem(2)],
        compiler_params=pltpu.CompilerParams(collective_id=0, has_side_effects=True, vmem_limit_bytes=VMEM_MAX),
        name='layer',
    )(x, lens, gains, freq, wq, wk, wv, wo, kc, vc, wg, wu, wd)


TILE = 1280
SUB = 320
SLOTS = 3


def head_epilogue(logits, diff, base):
    tv, n = logits.shape
    th = jnp.tanh(logits * (1.0 / FINAL_CAP)).reshape(tv // 8, 8, n)
    ex = jnp.exp2(th * (FINAL_CAP * LOG2E))
    rows = lax.broadcasted_iota(jnp.int32, th.shape, 0) * 8
    hit = jnp.where((diff - base)[None] == rows, th, 0.0)
    return jnp.sum(ex, axis=0), jnp.sum(hit, axis=0)


def head_kernel(y_own, gains, tgt, e_hbm, y_out, lp_ref,
                ag, yb, ht0, ht1, eb, lg_a, lg_b, dif, tot, hit, part, fin, e_sem, y_sem, s1, s2, s3, s4):
    t, v, tx, ty, tz = place()
    me = v * 4 + t
    dev_x, dev_y, dev_p = (tx, v), (ty, v), (t, 1 - v)
    g_fin = gains[4:5, :]
    tiles = e_hbm.shape[0] // TILE
    total = 2 * tiles

    def fetch(g):
        src = e_hbm.at[pl.ds(pl.multiple_of((g % tiles) * TILE, TILE), TILE)]
        return pltpu.make_async_copy(src, eb.at[g % SLOTS], e_sem.at[g % SLOTS])

    for g in range(SLOTS - 1):
        fetch(g).start()
    meet_all(t, v)

    first = [send(y_own.at[h], ag.at[h, me], s1, (i,), dev)
             for i, (h, dev) in enumerate(((0, dev_x), (1, dev_y), (1, dev_x), (0, dev_y)))]
    second = [send(ag.at[h, v * 4 + q], ag.at[h, v * 4 + q], s2, (h,), dev) for h, q, dev in ((0, tx, dev_y), (1, ty, dev_x))]
    cross = [send(y_own, ag.at[:, me], s3, (0,), dev_p)]
    cross += [send(ag.at[:, v * 4 + q], ag.at[:, v * 4 + q], s3, (i + 1,), dev_p) for i, q in enumerate((tx, ty, tz))]
    cross[0].start()
    for cp in first:
        cp.start()
    tot[...] = jnp.zeros_like(tot)
    hit[...] = jnp.zeros_like(hit)
    spots = [w * 4 + q for q in (t, tx, ty, tz) for w in range(2)]
    for k, b in enumerate(spots):
        lane = tgt[b] - me * e_hbm.shape[0]
        dif[:, OWN * k:OWN * k + OWN] = lane - lax.broadcasted_iota(jnp.int32, (8, OWN), 0)

    def y_copy(b):
        return pltpu.make_async_copy(yb.at[b], y_out.at[pl.ds(pl.multiple_of(b * OWN, OWN), OWN)], y_sem.at[b])

    def prepare(h_a, h_b, b, ht, lanes):
        yb[b, :, :COLS] = h_a.astype(BF16)
        yb[b, :, COLS:] = h_b.astype(BF16)
        y_copy(b).start()
        n_a, n_b = norm_halves(h_a, h_b, g_fin)
        ht[:COLS, lanes] = n_a.T.astype(BF16)
        ht[COLS:, lanes] = n_b.T.astype(BF16)

    cross[0].wait_recv()
    other = (1 - v) * 4 + t
    prepare(y_own[0], y_own[1], me, ht0, pl.ds(pl.multiple_of(v * OWN, OWN), OWN))
    prepare(ag[0, other], ag[1, other], other, ht0, pl.ds(pl.multiple_of((1 - v) * OWN, OWN), OWN))

    def epilogue(lg, span, base, valid):
        s, k = head_epilogue(lg, dif[:, span], base)
        tot[:, span] += jnp.where(valid, s, 0.0)
        hit[:, span] += jnp.where(valid, k, 0.0)

    def body(i, offset, ht, bufs, span):
        g = i + offset
        slot = g % SLOTS
        fetch(g).wait()

        @pl.when(g + SLOTS - 1 < total)
        def _():
            fetch(g + SLOTS - 1).start()

        for k in range(TILE // SUB):
            cur, prev = bufs[k % 2], bufs[(k + 1) % 2]
            cur[...] = jnp.dot(eb[slot, SUB * k:SUB * k + SUB, :], ht[...], preferred_element_type=F32)
            epilogue(prev[...], span, i * TILE + (k - 1) * SUB, True if k else i > 0)

    near, far = slice(0, 2 * OWN), slice(2 * OWN, 8 * OWN)
    near_bufs = (lg_a.at[:, near], lg_b.at[:, near])

    def pass_one(i, _):
        @pl.when(i == 9)
        def _():
            for cp, nxt in zip(first[:2], second):
                cp.wait_recv()
                nxt.start()

        @pl.when(i == 15)
        def _():
            for cp in first[2:]:
                cp.wait_recv()
            cross[1].start()
            cross[2].start()

        @pl.when(i == 17)
        def _():
            cross[1].wait_recv()
            cross[2].wait_recv()

        @pl.when((i >= 17) & (i < 21))
        def _():
            k = i - 17
            chip = tx + (k // 2) * (ty - tx)
            b = (k % 2) * 4 + chip
            prepare(ag[0, b], ag[1, b], b, ht1, pl.ds(pl.multiple_of(k * OWN, OWN), OWN))

        @pl.when(i == 23)
        def _():
            for cp in second:
                cp.wait_recv()
            cross[3].start()

        body(i, 0, ht0, near_bufs, near)
        return 0

    lax.fori_loop(0, tiles, pass_one, 0)
    epilogue(lg_b[:, near], near, tiles * TILE - SUB, True)
    cross[3].wait_recv()
    for k in (4, 5):
        b = (k % 2) * 4 + tz
        prepare(ag[0, b], ag[1, b], b, ht1, slice(OWN * k, OWN * k + OWN))
    lax.fori_loop(0, tiles, lambda i, _: (body(i, tiles, ht1, (lg_a, lg_b), far), 0)[1], 0)
    epilogue(lg_b[...], far, tiles * TILE - SUB, True)

    for k, b in enumerate(spots):
        lanes = slice(OWN * k, OWN * k + OWN)
        part[b, 0:1] = jnp.sum(tot[:, lanes], axis=0, keepdims=True)
        part[b, 1:2] = jnp.sum(hit[:, lanes], axis=0, keepdims=True)
    outs = []
    for k in range(1, 8):
        dt, dv = k % 4, k // 4
        outs.append(send(part, fin.at[k], s4, (k - 1,), ((t + dt) % 4, (v + dv) % 2)))
    for cp in outs:
        cp.start()
    acc = part[...]
    for k in range(1, 8):
        outs[k - 1].wait_recv()
        acc += fin[k]
    lp_ref[...] = FINAL_CAP * acc[:, 1] - jnp.log(acc[:, 0])
    for cp in first + second + cross + outs:
        cp.wait_send()
    for b in range(8):
        y_copy(b).wait()


def head(y_own, gains, tgt, table):
    d = table.shape[1]
    vm, hbm = pl.BlockSpec(memory_space=pltpu.VMEM), pl.BlockSpec(memory_space=pl.ANY)
    return pl.pallas_call(
        head_kernel,
        out_shape=[jax.ShapeDtypeStruct((8 * OWN, d), BF16), jax.ShapeDtypeStruct((8, OWN), F32)],
        in_specs=[vm, vm, vm, hbm],
        out_specs=[hbm, vm],
        scratch_shapes=[
            pltpu.VMEM((2, 8, OWN, COLS), F32), pltpu.VMEM((8, OWN, d), BF16), pltpu.VMEM((d, 256), BF16), pltpu.VMEM((d, 768), BF16),
            pltpu.VMEM((SLOTS, TILE, d), BF16), pltpu.VMEM((SUB, 768), F32), pltpu.VMEM((SUB, 768), F32),
            pltpu.VMEM((8, 8 * OWN), jnp.int32), pltpu.VMEM((8, 8 * OWN), F32), pltpu.VMEM((8, 8 * OWN), F32),
            pltpu.VMEM((8, 2, OWN), F32), pltpu.VMEM((8, 8, 2, OWN), F32),
            pltpu.SemaphoreType.DMA((SLOTS,)), pltpu.SemaphoreType.DMA((8,)),
            pltpu.SemaphoreType.DMA((2, 4)), pltpu.SemaphoreType.DMA((2, 2)), pltpu.SemaphoreType.DMA((2, 4)), pltpu.SemaphoreType.DMA((2, 7))],
        compiler_params=pltpu.CompilerParams(collective_id=1, has_side_effects=True, vmem_limit_bytes=VMEM_MAX),
        name='head',
    )(y_own, gains, tgt, table)


def solution(mesh):
    in_specs = (P(), P(), P(), P(), P(None, 't'), P(None, 't'), P(None, 't'), P('t', None), P(), P(), P(None, 't'), P(None, 't'), P('t', None), P(), P(), P(None, None, 't', None), P(None, None, 't', None), P(('v', 't'), None))

    def local_step(hidden_in, seq_lens, target, g_attn_pre, w_q, w_k, w_v, w_o, g_attn_post, g_mlp_pre, w_gate, w_up, w_down, g_mlp_post, g_final, k_cache, v_cache, embed_table):
        picks = lax.broadcasted_iota(jnp.int32, (5, hidden_in.shape[1]), 0)
        gains = g_final[None]
        for i, g in enumerate((g_attn_pre, g_attn_post, g_mlp_pre, g_mlp_post)):
            gains = jnp.where(picks == i, g[None], gains)
        gains = gains.astype(F32)
        freq = jnp.asarray((ROPE_BASE ** (-2.0 * np.arange(128, dtype=np.float32) / 256)).astype(np.float32)[None])
        y_own = layer(hidden_in, seq_lens.reshape(8, 1, OWN), gains, freq, w_q, w_k, w_v, w_o,
                      k_cache.reshape(-1, 256), v_cache.reshape(-1, 256), w_gate, w_up, w_down)
        hidden_out, logprob = head(y_own, gains, target.reshape(8, 1, OWN), embed_table)
        return logprob.reshape(-1), hidden_out

    return jax.shard_map(local_step, mesh=mesh, in_specs=in_specs, out_specs=(P(), P()), check_vma=False)
```

```python
import jax
import jax.numpy as jnp
import numpy as np
from jax import lax
from jax.experimental import pallas as pl
from jax.experimental.pallas import tpu as pltpu
from jax.sharding import PartitionSpec as P

ATTN_CAP = 50.0
FINAL_CAP = 30.0
NORM_EPS = 1e-6
ROPE_BASE = 10000.0
LOG2E = 1.4426950408889634
BF16 = jnp.bfloat16
F32 = jnp.float32
VMEM_LIMIT = 60 * 1024 * 1024
VMEM_MAX = 67043328


def rms_norm(values, gain_vec):
    x_f32 = values.astype(F32)
    scaled = x_f32 * lax.rsqrt(jnp.mean(x_f32 * x_f32, axis=-1, keepdims=True) + NORM_EPS)
    return scaled * (1.0 + gain_vec.astype(F32))


def rope(vec, cos_t, sin_t):
    low, high = vec[:, :128], vec[:, 128:]
    out = jnp.concatenate([low * cos_t - high * sin_t, high * cos_t + low * sin_t], axis=1)
    return out.astype(BF16).astype(F32)


def attend(x, lens, gain, freq, wq, wk, wv, wo, keys, vals, put):
    tb = x.shape[0]
    groups = tb // 8
    scale = 1.0 / (16.0 * ATTN_CAP)
    a = rms_norm(x, gain).astype(BF16)
    q = jnp.dot(a, wq, preferred_element_type=F32)
    k = jnp.dot(a, wk, preferred_element_type=F32)
    v = jnp.dot(a, wv, preferred_element_type=F32).astype(BF16).astype(F32)
    ang = lens.astype(F32) * freq
    cos_t, sin_t = jnp.cos(ang), jnp.sin(ang)

    def pairs(first, second):
        both = jnp.stack([first.reshape(groups, 8, -1), second.reshape(groups, 8, -1)], axis=1)
        return both.reshape(2 * tb, first.shape[1])

    q_all = pairs(rope(q[:, :256], cos_t, sin_t), rope(q[:, 256:], cos_t, sin_t))
    k = rope(k, cos_t, sin_t)
    k_all, v_all, len_all = pairs(k, k), pairs(v, v), pairs(lens, lens)
    q_b = q_all.astype(BF16)
    nt = (((1,), (1,)), ((), ()))
    s = jnp.concatenate([lax.dot_general(q_b[16 * i:16 * i + 16], keys(i), nt, preferred_element_type=F32)
                         for i in range(groups)], axis=0)
    s = ATTN_CAP * jnp.tanh(s * scale)
    row = lax.broadcasted_iota(jnp.int32, s.shape, 0)
    col = lax.broadcasted_iota(jnp.int32, s.shape, 1)
    rel = col - (row % 8) * 32
    s = jnp.where((rel >= 0) & (rel < len_all), s, -1e30)
    s_new = ATTN_CAP * jnp.tanh(jnp.sum(q_all * k_all, axis=1, keepdims=True) * scale)
    top = jnp.maximum(jnp.max(s, axis=1, keepdims=True), s_new)
    e = jnp.exp(s - top)
    e_new = jnp.exp(s_new - top)
    den = jnp.sum(e, axis=1, keepdims=True) + e_new
    e_b = e.astype(BF16)
    o = jnp.concatenate([jnp.dot(e_b[16 * i:16 * i + 16], vals(i), preferred_element_type=F32) for i in range(groups)], axis=0)
    o = ((o + e_new.astype(BF16).astype(F32) * v_all) / den).reshape(groups, 2, 8, 256)
    o_b = jnp.concatenate([o[:, 0].reshape(tb, 256), o[:, 1].reshape(tb, 256)], axis=1).astype(BF16)
    for j in range(wo.shape[1] // 384):
        put(j, jnp.dot(o_b, wo[:, 384 * j:384 * j + 384], preferred_element_type=F32))


MESH = pl.DeviceIdType.MESH
CHUNKS = 4
OWN = 128
PART = OWN // CHUNKS
COLS = 1152


def place():
    t, v = lax.axis_index('t'), lax.axis_index('v')
    return t, v, t + 1 - 2 * (t % 2), (t + 2) % 4, 3 - t


def meet_all(t, v):
    barrier = pltpu.get_barrier_semaphore()
    for dt in range(4):
        for dv in range(2):
            if dt or dv:
                pl.semaphore_signal(barrier, inc=1, device_id=((t + dt) % 4, (v + dv) % 2), device_id_type=MESH)
    pl.semaphore_wait(barrier, 7)


def send(src, dst, sems, idx, dev):
    return pltpu.make_async_remote_copy(src_ref=src, dst_ref=dst, send_sem=sems.at[(0,) + idx], recv_sem=sems.at[(1,) + idx],
                                        device_id=dev, device_id_type=MESH)


def norm_halves(h0, h1, g_ref):
    d = 2 * h0.shape[1]
    inv = lax.rsqrt((jnp.sum(h0 * h0, axis=1, keepdims=True) + jnp.sum(h1 * h1, axis=1, keepdims=True)) / d + NORM_EPS)
    return h0 * inv * (1.0 + g_ref[:, :COLS]), h1 * inv * (1.0 + g_ref[:, COLS:])


TILE = 1280
SUB = 320
SLOTS = 4


def head_epilogue(logits, diff, base):
    tv, n = logits.shape
    th = jnp.tanh(logits * (1.0 / FINAL_CAP)).reshape(tv // 8, 8, n)
    ex = jnp.exp2(th * (FINAL_CAP * LOG2E))
    rows = lax.broadcasted_iota(jnp.int32, th.shape, 0) * 8
    hit = jnp.where((diff - base)[None] == rows, th, 0.0)
    return jnp.sum(ex, axis=0), jnp.sum(hit, axis=0)


def step_kernel(x_hbm, lens, gains, freq, tgt, wq_hbm, wk_hbm, wv_hbm, wo_hbm, kc_hbm, vc_hbm, wg_hbm, wu_hbm, wd_hbm, e_hbm, y_out, lp_ref,
                bank, xh, x1, p1, r1, r2, fwd, ag, p2, mb, act, lens_s, ht0, ht1, lg_a, lg_b, dif, tot, hit, sums, fin,
                loads, caches, e_sem, y_sem, s1, s2, s3, s4, s5, s6, s7, s8, s9, s10, s11, free_sem):
    t, v, tx, ty, tz = place()
    dev_x, dev_y = (tx, v), (ty, v)
    g_post, g_pre, g_mlp, g_fin = gains[1:2, :], gains[2:3, :], gains[3:4, :], gains[4:5, :]
    d = xh.shape[1]
    rows = lambda q, c: pl.ds(pl.multiple_of(q * OWN + c * PART, PART), PART)
    part = lambda c: pl.ds(pl.multiple_of(c * PART, PART), PART)
    wq, wk, wv, wo = bank.at[:d, :512], bank.at[:d, 512:768], bank.at[:d, 768:1024], bank.at[d:d + 512]
    cache_row = d + 512
    wg, wu, wd = bank.at[:d], bank.at[d:2 * d], bank.at[2 * d:]
    local = pltpu.make_async_copy
    early = [local(a, b, loads.at[i]) for i, (a, b) in enumerate((
        (x_hbm.at[pl.ds(pl.multiple_of(v * 4 * OWN, 4 * OWN), 4 * OWN)], xh), (wq_hbm, wq), (wk_hbm, wk), (wv_hbm, wv)))]
    wo_load = local(wo_hbm, wo, loads.at[4])
    weights = [local(a, b, loads.at[5 + i]) for i, (a, b) in enumerate(((wg_hbm, wg), (wu_hbm, wu), (wd_hbm, wd)))]

    def cache_load(c):
        out = []
        for i, src in enumerate((kc_hbm, vc_hbm)):
            for q in range(4):
                first = pl.multiple_of(((v * 4 + q) * OWN + c * PART) * 32, PART * 32)
                out.append(local(src.at[pl.ds(first, PART * 32)],
                                 bank.at[pl.ds(cache_row + q * PART * 32, PART * 32), pl.ds(pl.multiple_of((2 * c + i) * 256, 256), 256)],
                                 caches.at[c, 4 * i + q]))
        return out

    for cp in early:
        cp.start()
    for cp in cache_load(0):
        cp.start()
    wo_load.start()
    for c in range(1, CHUNKS):
        for cp in cache_load(c):
            cp.start()
    for q in range(4):
        lens_s[OWN * q:OWN * q + OWN, :] = jnp.broadcast_to(lens[v * 4 + q], (OWN, OWN)).T
    meet_all(t, v)
    for cp in early:
        cp.wait()

    def rs_first(p, r, sems, c):
        return [send(p.at[h, rows(q, c)], r.at[h, slot, part(c)], sems, (c, 2 * h + slot), dev)
                for h, slot, q, dev in ((0, 1, tz, dev_x), (1, 1, tz, dev_y), (0, 0, tx, dev_x), (1, 0, ty, dev_y))]

    def rs_second(r, sems, c):
        return [send(fwd.at[h, part(c)], r.at[h, part(c)], sems, (c, h), dev) for h, dev in ((0, dev_y), (1, dev_x))]

    def rs_forward(p, r, r_next, sems, sems_next, c):
        first = rs_first(p, r, sems, c)
        for h, q, cp in ((0, ty, rs_second(r_next, sems_next, c)[0]), (1, tx, rs_second(r_next, sems_next, c)[1])):
            first[h].wait_recv()
            fwd[h, part(c)] = p[h, rows(q, c)] + r[h, 1, part(c)]
            cp.start()

    def rs_finish(p, r, r_next, sems, sems_next, c):
        first, second = rs_first(p, r, sems, c), rs_second(r_next, sems_next, c)
        out = []
        for h in range(2):
            first[2 + h].wait_recv()
            second[h].wait_recv()
            out.append(p[h, rows(t, c)] + r[h, 0, part(c)] + r_next[h, part(c)])
        for cp in first + second:
            cp.wait_send()
        return out

    def ag_first(c, sems):
        return [send(ag.at[h, rows(t, c)], ag.at[h, rows(t, c)], sems, (c, i), dev)
                for i, (h, dev) in enumerate(((0, dev_x), (1, dev_y), (1, dev_x), (0, dev_y)))]

    def ag_second(c, sems):
        return [send(ag.at[h, rows(q, c)], ag.at[h, rows(q, c)], sems, (c, h), dev) for h, q, dev in ((0, tx, dev_y), (1, ty, dev_x))]

    def each(body):
        lax.fori_loop(0, CHUNKS, lambda c, _: (body(c), 0)[1], 0)

    @each
    def _(c):
        for cp in cache_load(c):
            cp.wait()

        @pl.when(c == 0)
        def _():
            wo_load.wait()

        x = jnp.concatenate([xh[rows(q, c), :] for q in range(4)], axis=0)
        lens_c = jnp.concatenate([lens_s[rows(q, c), :1] for q in range(4)], axis=0)

        def cached(i):
            return lambda g: bank[pl.ds(cache_row + 256 * g, 256), pl.ds(pl.multiple_of((2 * c + i) * 256, 256), 256)]

        def put(j, res):
            h, first = j // 3, 384 * (j % 3)
            for q in range(4):
                p1[h, rows(q, c), first:first + 384] = res[PART * q:PART * q + PART]

        attend(x, lens_c, gains[0:1, :], freq[...], wq[...], wk[...], wv[...], wo, cached(0), cached(1), put)
        for cp in rs_first(p1, r1, s1, c):
            cp.start()

    for w in weights:
        w.start()

    @each
    def _(c):
        rs_forward(p1, r1, r2, s1, s2, c)

    @each
    def _(c):
        s_a, s_b = norm_halves(*rs_finish(p1, r1, r2, s1, s2, c), g_post)
        x_a = (xh[rows(t, c), :COLS].astype(F32) + s_a).astype(BF16)
        x_b = (xh[rows(t, c), COLS:].astype(F32) + s_b).astype(BF16)
        x1[part(c), :COLS] = x_a
        x1[part(c), COLS:] = x_b
        m_a, m_b = norm_halves(x_a.astype(F32), x_b.astype(F32), g_pre)
        ag[0, rows(t, c)] = m_a.astype(BF16).astype(F32)
        ag[1, rows(t, c)] = m_b.astype(BF16).astype(F32)
        for cp in ag_first(c, s3):
            cp.start()

    @each
    def _(c):
        for cp, nxt in zip(ag_first(c, s3)[:2], ag_second(c, s4)):
            cp.wait_recv()
            nxt.start()

    pl.semaphore_signal(free_sem, inc=1, device_id=(t, 1 - v), device_id_type=MESH)
    for w in weights:
        w.wait()

    @each
    def _(c):
        for cp in ag_first(c, s3)[2:] + ag_second(c, s4):
            cp.wait_recv()
        for cp in ag_first(c, s3) + ag_second(c, s4):
            cp.wait_send()
        for q in range(4):
            for h in range(2):
                mb[PART * q:PART * q + PART, COLS * h:COLS * h + COLS] = ag[h, rows(q, c)].astype(BF16)

        def up(j, _):
            cols = pl.ds(pl.multiple_of(j * 256, 256), 256)
            gate = jnp.dot(mb[...], wg[:, cols], preferred_element_type=F32)
            lift = jnp.dot(mb[...], wu[:, cols], preferred_element_type=F32)
            act[:, cols] = (jax.nn.gelu(gate, approximate=True) * lift).astype(BF16)
            return 0

        lax.fori_loop(0, d // 256, up, 0)
        for h in range(2):
            def down(j, _):
                res = jnp.dot(act[...], wd[:, pl.ds(pl.multiple_of(COLS * h + j * 384, 128), 384)], preferred_element_type=F32)
                for q in range(4):
                    p2[h, rows(q, c), pl.ds(pl.multiple_of(j * 384, 128), 384)] = res[PART * q:PART * q + PART]
                return 0

            lax.fori_loop(0, COLS // 384, down, 0)
        for cp in rs_first(p2, r1, s5, c):
            cp.start()

    me, oth = v * 4 + t, p1
    eb = bank.at[:SLOTS * TILE]
    yb = bank.at[SLOTS * TILE:SLOTS * TILE + 8 * OWN]
    tiles = e_hbm.shape[0] // TILE
    total = 2 * tiles

    def slot_of(g):
        return pl.ds(pl.multiple_of((g % SLOTS) * TILE, TILE), TILE)

    def fetch(g):
        src = e_hbm.at[pl.ds(pl.multiple_of((g % tiles) * TILE, TILE), TILE)]
        return local(src, eb.at[slot_of(g)], e_sem.at[g % SLOTS])

    for g in range(SLOTS):
        fetch(g).start()

    @each
    def _(c):
        rs_forward(p2, r1, r2, s5, s6, c)

    def cross_own(c):
        return send(ag.at[:, rows(t, c)], oth.at[:, rows(t, c)], s9, (c,), (t, 1 - v))

    pl.semaphore_wait(free_sem, 1)

    @each
    def _(c):
        s_a, s_b = norm_halves(*rs_finish(p2, r1, r2, s5, s6, c), g_mlp)
        ag[0, rows(t, c)] = (x1[part(c), :COLS].astype(F32) + s_a).astype(BF16).astype(F32)
        ag[1, rows(t, c)] = (x1[part(c), COLS:].astype(F32) + s_b).astype(BF16).astype(F32)
        cross_own(c).start()
        for cp in ag_first(c, s7):
            cp.start()

    block = lambda q: pl.ds(pl.multiple_of(q * OWN, OWN), OWN)
    cross = [send(ag.at[:, block(q)], oth.at[:, block(q)], s10, (i,), (t, 1 - v)) for i, q in enumerate((tx, ty, tz))]
    tot[...] = jnp.zeros_like(tot)
    hit[...] = jnp.zeros_like(hit)
    spots = [w * 4 + q for q in (t, tx, ty, tz) for w in (v, 1 - v)]
    for k, b in enumerate(spots):
        lane = tgt[b] - me * e_hbm.shape[0]
        dif[:, OWN * k:OWN * k + OWN] = lane - lax.broadcasted_iota(jnp.int32, (8, OWN), 0)

    def y_copy(b):
        return local(yb.at[block(b)], y_out.at[block(b)], y_sem.at[b])

    def prepare(src, w, q, ht, lanes):
        h_a, h_b = src[0, block(q)], src[1, block(q)]
        b = w * 4 + q
        yb[block(b), :COLS] = h_a.astype(BF16)
        yb[block(b), COLS:] = h_b.astype(BF16)
        y_copy(b).start()
        n_a, n_b = norm_halves(h_a, h_b, g_fin)
        ht[:COLS, lanes] = n_a.T.astype(BF16)
        ht[COLS:, lanes] = n_b.T.astype(BF16)

    prepare(ag, v, t, ht0, slice(0, OWN))

    @each
    def _(c):
        cross_own(c).wait_recv()

    prepare(oth, 1 - v, t, ht0, slice(OWN, 2 * OWN))

    def epilogue(lg, span, base, valid):
        s, k = head_epilogue(lg, dif[:, span], base)
        tot[:, span] += jnp.where(valid, s, 0.0)
        hit[:, span] += jnp.where(valid, k, 0.0)

    def body(i, offset, ht, bufs, span):
        g = i + offset
        fetch(g).wait()

        @pl.when((g >= 1) & (g + SLOTS - 1 < total))
        def _():
            fetch(g + SLOTS - 1).start()

        first = pl.multiple_of((g % SLOTS) * TILE, TILE)
        for k in range(TILE // SUB):
            cur, prev = bufs[k % 2], bufs[(k + 1) % 2]
            cur[...] = jnp.dot(bank[pl.ds(first + SUB * k, SUB), :], ht[...], preferred_element_type=F32)
            epilogue(prev[...], span, i * TILE + (k - 1) * SUB, True if k else i > 0)

    near, far = slice(0, 2 * OWN), slice(2 * OWN, 8 * OWN)
    near_bufs = (lg_a.at[:, near], lg_b.at[:, near])

    def pass_one(i, _):
        @pl.when((i >= 3) & (i < 15) & (i % 3 == 0))
        def _():
            c = i // 3 - 1
            for cp, nxt in zip(ag_first(c, s7)[:2], ag_second(c, s8)):
                cp.wait_recv()
                nxt.start()

        @pl.when(i == 16)
        def _():
            for c in range(CHUNKS):
                for cp in ag_first(c, s7)[2:]:
                    cp.wait_recv()
            cross[0].start()
            cross[1].start()

        @pl.when((i == 18) | (i == 20))
        def _():
            k = i - 18
            prepare(ag, v, tx + (k // 2) * (ty - tx), ht1, pl.ds(pl.multiple_of(k * OWN, OWN), OWN))

        @pl.when(i == 19)
        def _():
            cross[0].wait_recv()
            cross[1].wait_recv()

        @pl.when((i == 19) | (i == 21))
        def _():
            k = i - 18
            prepare(oth, 1 - v, tx + (k // 2) * (ty - tx), ht1, pl.ds(pl.multiple_of(k * OWN, OWN), OWN))

        @pl.when(i == 23)
        def _():
            for c in range(CHUNKS):
                for cp in ag_second(c, s8):
                    cp.wait_recv()
            cross[2].start()

        body(i, 0, ht0, near_bufs, near)
        return 0

    lax.fori_loop(0, tiles, pass_one, 0)
    epilogue(lg_b[:, near], near, tiles * TILE - SUB, True)
    prepare(ag, v, tz, ht1, slice(4 * OWN, 5 * OWN))
    cross[2].wait_recv()
    prepare(oth, 1 - v, tz, ht1, slice(5 * OWN, 6 * OWN))
    lax.fori_loop(0, tiles, lambda i, _: (body(i, tiles, ht1, (lg_a, lg_b), far), 0)[1], 0)
    epilogue(lg_b[...], far, tiles * TILE - SUB, True)

    for k, b in enumerate(spots):
        lanes = slice(OWN * k, OWN * k + OWN)
        sums[b, 0:1] = jnp.sum(tot[:, lanes], axis=0, keepdims=True)
        sums[b, 1:2] = jnp.sum(hit[:, lanes], axis=0, keepdims=True)
    outs = []
    for k in range(1, 8):
        dt, dv = k % 4, k // 4
        outs.append(send(sums, fin.at[k], s11, (k - 1,), ((t + dt) % 4, (v + dv) % 2)))
    for cp in outs:
        cp.start()
    acc = sums[...]
    for k in range(1, 8):
        outs[k - 1].wait_recv()
        acc += fin[k]
    lp_ref[...] = FINAL_CAP * acc[:, 1] - jnp.log(acc[:, 0])
    for c in range(CHUNKS):
        for cp in ag_first(c, s7) + ag_second(c, s8) + [cross_own(c)]:
            cp.wait_send()
    for cp in cross + outs:
        cp.wait_send()
    for b in range(8):
        y_copy(b).wait()


def step(x, lens, gains, freq, tgt, wq, wk, wv, wo, kc, vc, wg, wu, wd, table):
    d = x.shape[1]
    n = x.shape[0] // 2
    vm, hbm = pl.BlockSpec(memory_space=pltpu.VMEM), pl.BlockSpec(memory_space=pl.ANY)
    sem = lambda *k: pltpu.SemaphoreType.DMA(k)
    return pl.pallas_call(
        step_kernel,
        out_shape=[jax.ShapeDtypeStruct(x.shape, BF16), jax.ShapeDtypeStruct((8, OWN), F32)],
        in_specs=[hbm, vm, vm, vm, vm] + [hbm] * 10,
        out_specs=[hbm, vm],
        scratch_shapes=[
            pltpu.VMEM((3 * d, d), BF16), pltpu.VMEM((n, d), BF16), pltpu.VMEM((OWN, d), BF16), pltpu.VMEM((2, n, COLS), F32),
            pltpu.VMEM((2, 2, OWN, COLS), F32), pltpu.VMEM((2, OWN, COLS), F32),
            pltpu.VMEM((2, OWN, COLS), F32), pltpu.VMEM((2, n, COLS), F32), pltpu.VMEM((2, n, COLS), F32),
            pltpu.VMEM((OWN, d), BF16), pltpu.VMEM((OWN, d), BF16), pltpu.VMEM((n, 128), jnp.int32),
            pltpu.VMEM((d, 256), BF16), pltpu.VMEM((d, 768), BF16), pltpu.VMEM((SUB, 768), F32), pltpu.VMEM((SUB, 768), F32),
            pltpu.VMEM((8, 8 * OWN), jnp.int32), pltpu.VMEM((8, 8 * OWN), F32), pltpu.VMEM((8, 8 * OWN), F32),
            pltpu.VMEM((8, 2, OWN), F32), pltpu.VMEM((8, 8, 2, OWN), F32),
            sem(8), sem(CHUNKS, 8), sem(SLOTS), sem(8),
            sem(2, CHUNKS, 4), sem(2, CHUNKS, 2), sem(2, CHUNKS, 4), sem(2, CHUNKS, 2), sem(2, CHUNKS, 4), sem(2, CHUNKS, 2),
            sem(2, CHUNKS, 4), sem(2, CHUNKS, 2), sem(2, CHUNKS), sem(2, 3), sem(2, 7), pltpu.SemaphoreType.REGULAR],
        compiler_params=pltpu.CompilerParams(collective_id=0, has_side_effects=True, vmem_limit_bytes=VMEM_MAX),
        name='step',
    )(x, lens, gains, freq, tgt, wq, wk, wv, wo, kc, vc, wg, wu, wd, table)


def finish_kernel(y_hbm, lp_ref, y_out, lp_out, yb, sems):
    blocks = yb.shape[0]
    rows = yb.shape[1]
    take = [pltpu.make_async_copy(y_hbm.at[rows * i:rows * i + rows], yb.at[i], sems.at[0, i]) for i in range(blocks)]
    give = [pltpu.make_async_copy(yb.at[i], y_out.at[rows * i:rows * i + rows], sems.at[1, i]) for i in range(blocks)]
    for cp in take:
        cp.start()
    lp_out[...] = lp_ref[...]
    for a, b in zip(take, give):
        a.wait()
        b.start()
    for cp in give:
        cp.wait()


def finish(y, lp):
    vm, hbm = pl.BlockSpec(memory_space=pltpu.VMEM), pl.BlockSpec(memory_space=pl.ANY)
    return pl.pallas_call(
        finish_kernel,
        out_shape=[jax.ShapeDtypeStruct(y.shape, y.dtype), jax.ShapeDtypeStruct(lp.shape, lp.dtype)],
        in_specs=[hbm, vm],
        out_specs=[hbm, vm],
        scratch_shapes=[pltpu.VMEM((8, y.shape[0] // 8, y.shape[1]), y.dtype), pltpu.SemaphoreType.DMA((2, 8))],
        compiler_params=pltpu.CompilerParams(vmem_limit_bytes=VMEM_LIMIT),
        name='finish',
    )(y, lp)


def solution(mesh):
    in_specs = (P(), P(), P(), P(), P(None, 't'), P(None, 't'), P(None, 't'), P('t', None), P(), P(), P(None, 't'), P(None, 't'), P('t', None), P(), P(), P(None, None, 't', None), P(None, None, 't', None), P(('v', 't'), None))

    def local_step(hidden_in, seq_lens, target, g_attn_pre, w_q, w_k, w_v, w_o, g_attn_post, g_mlp_pre, w_gate, w_up, w_down, g_mlp_post, g_final, k_cache, v_cache, embed_table):
        picks = lax.broadcasted_iota(jnp.int32, (5, hidden_in.shape[1]), 0)
        gains = g_final[None]
        for i, g in enumerate((g_attn_pre, g_attn_post, g_mlp_pre, g_mlp_post)):
            gains = jnp.where(picks == i, g[None], gains)
        gains = gains.astype(F32)
        freq = jnp.asarray((ROPE_BASE ** (-2.0 * np.arange(128, dtype=np.float32) / 256)).astype(np.float32)[None])
        hidden_out, logprob = step(hidden_in, seq_lens.reshape(8, 1, OWN), gains, freq, target.reshape(8, 1, OWN), w_q, w_k, w_v, w_o,
                      k_cache.reshape(-1, 256), v_cache.reshape(-1, 256), w_gate, w_up, w_down, embed_table)
        hidden_out, logprob = finish(hidden_out, logprob)
        return logprob.reshape(-1), hidden_out

    return jax.shard_map(local_step, mesh=mesh, in_specs=in_specs, out_specs=(P(), P()), check_vma=False)
```

```python
import jax
import jax.numpy as jnp
import numpy as np
from jax import lax
from jax.experimental import pallas as pl
from jax.experimental.pallas import tpu as pltpu
from jax.sharding import PartitionSpec as P

ATTN_CAP = 50.0
FINAL_CAP = 30.0
NORM_EPS = 1e-6
ROPE_BASE = 10000.0
LOG2E = 1.4426950408889634
BF16 = jnp.bfloat16
F32 = jnp.float32
VMEM_LIMIT = 60 * 1024 * 1024
VMEM_MAX = 67043328


def rms_norm(values, gain_vec):
    x_f32 = values.astype(F32)
    scaled = x_f32 * lax.rsqrt(jnp.mean(x_f32 * x_f32, axis=-1, keepdims=True) + NORM_EPS)
    return scaled * (1.0 + gain_vec.astype(F32))


def rope(vec, cos_t, sin_t):
    low, high = vec[:, :128], vec[:, 128:]
    out = jnp.concatenate([low * cos_t - high * sin_t, high * cos_t + low * sin_t], axis=1)
    return out.astype(BF16).astype(F32)


def attend(x, lens, gain, freq, wq, wk, wv, wo, keys, vals, put):
    tb = x.shape[0]
    groups = tb // 8
    scale = 1.0 / (16.0 * ATTN_CAP)
    a = rms_norm(x, gain).astype(BF16)
    q = jnp.dot(a, wq, preferred_element_type=F32)
    k = jnp.dot(a, wk, preferred_element_type=F32)
    v = jnp.dot(a, wv, preferred_element_type=F32).astype(BF16).astype(F32)
    ang = lens.astype(F32) * freq
    cos_t, sin_t = jnp.cos(ang), jnp.sin(ang)

    def pairs(first, second):
        both = jnp.stack([first.reshape(groups, 8, -1), second.reshape(groups, 8, -1)], axis=1)
        return both.reshape(2 * tb, first.shape[1])

    q_all = pairs(rope(q[:, :256], cos_t, sin_t), rope(q[:, 256:], cos_t, sin_t))
    k = rope(k, cos_t, sin_t)
    k_all, v_all, len_all = pairs(k, k), pairs(v, v), pairs(lens, lens)
    q_b = q_all.astype(BF16)
    nt = (((1,), (1,)), ((), ()))
    s = jnp.concatenate([lax.dot_general(q_b[16 * i:16 * i + 16], keys(i), nt, preferred_element_type=F32)
                         for i in range(groups)], axis=0)
    s = ATTN_CAP * jnp.tanh(s * scale)
    row = lax.broadcasted_iota(jnp.int32, s.shape, 0)
    col = lax.broadcasted_iota(jnp.int32, s.shape, 1)
    rel = col - (row % 8) * 32
    s = jnp.where((rel >= 0) & (rel < len_all), s, -1e30)
    s_new = ATTN_CAP * jnp.tanh(jnp.sum(q_all * k_all, axis=1, keepdims=True) * scale)
    top = jnp.maximum(jnp.max(s, axis=1, keepdims=True), s_new)
    e = jnp.exp(s - top)
    e_new = jnp.exp(s_new - top)
    den = jnp.sum(e, axis=1, keepdims=True) + e_new
    e_b = e.astype(BF16)
    o = jnp.concatenate([jnp.dot(e_b[16 * i:16 * i + 16], vals(i), preferred_element_type=F32) for i in range(groups)], axis=0)
    o = ((o + e_new.astype(BF16).astype(F32) * v_all) / den).reshape(groups, 2, 8, 256)
    o_b = jnp.concatenate([o[:, 0].reshape(tb, 256), o[:, 1].reshape(tb, 256)], axis=1).astype(BF16)
    for j in range(wo.shape[1] // 384):
        put(j, jnp.dot(o_b, wo[:, 384 * j:384 * j + 384], preferred_element_type=F32))


MESH = pl.DeviceIdType.MESH
CHUNKS = 4
OWN = 128
PART = OWN // CHUNKS
COLS = 1152


def place():
    t, v = lax.axis_index('t'), lax.axis_index('v')
    return t, v, t + 1 - 2 * (t % 2), (t + 2) % 4, 3 - t


def meet_all(t, v):
    barrier = pltpu.get_barrier_semaphore()
    for dt in range(4):
        for dv in range(2):
            if dt or dv:
                pl.semaphore_signal(barrier, inc=1, device_id=((t + dt) % 4, (v + dv) % 2), device_id_type=MESH)
    pl.semaphore_wait(barrier, 7)


def send(src, dst, sems, idx, dev):
    return pltpu.make_async_remote_copy(src_ref=src, dst_ref=dst, send_sem=sems.at[(0,) + idx], recv_sem=sems.at[(1,) + idx],
                                        device_id=dev, device_id_type=MESH)


def norm_halves(h0, h1, g_ref):
    d = 2 * h0.shape[1]
    inv = lax.rsqrt((jnp.sum(h0 * h0, axis=1, keepdims=True) + jnp.sum(h1 * h1, axis=1, keepdims=True)) / d + NORM_EPS)
    return h0 * inv * (1.0 + g_ref[:, :COLS]), h1 * inv * (1.0 + g_ref[:, COLS:])


TILE = 1280
SUB = 320
SLOTS = 4


def head_epilogue(logits, diff, base):
    tv, n = logits.shape
    th = jnp.tanh(logits * (1.0 / FINAL_CAP)).reshape(tv // 8, 8, n)
    ex = jnp.exp2(th * (FINAL_CAP * LOG2E))
    rows = lax.broadcasted_iota(jnp.int32, th.shape, 0) * 8
    hit = jnp.where((diff - base)[None] == rows, th, 0.0)
    return jnp.sum(ex, axis=0), jnp.sum(hit, axis=0)


def step_kernel(x_hbm, lens, ga, gb, gc, gd, ge, freq, tgt, wq_hbm, wk_hbm, wv_hbm, wo_hbm, kc_hbm, vc_hbm, wg_hbm, wu_hbm, wd_hbm, e_hbm, y_out, lp_ref,
                bank, xh, x1, p1, r1, r2, fwd, ag, p2, mb, act, gains, lens_s, ht0, ht1, lg_a, lg_b, dif, tot, hit, sums, fin,
                loads, caches, e_sem, y_sem, s1, s2, s3, s4, s5, s6, s7, s8, s9, s10, s11, free_sem):
    t, v, tx, ty, tz = place()
    dev_x, dev_y = (tx, v), (ty, v)
    for i, g in enumerate((ga, gb, gc, gd, ge)):
        gains[i:i + 1, :] = g[...].astype(F32).reshape(1, -1)
    g_post, g_pre, g_mlp, g_fin = gains[1:2, :], gains[2:3, :], gains[3:4, :], gains[4:5, :]
    d = xh.shape[1]
    rows = lambda q, c: pl.ds(pl.multiple_of(q * OWN + c * PART, PART), PART)
    part = lambda c: pl.ds(pl.multiple_of(c * PART, PART), PART)
    wq, wk, wv, wo = bank.at[:d, :512], bank.at[:d, 512:768], bank.at[:d, 768:1024], bank.at[d:d + 512]
    cache_row = d + 512
    wg, wu, wd = bank.at[:d], bank.at[d:2 * d], bank.at[2 * d:]
    local = pltpu.make_async_copy
    early = [local(a, b, loads.at[i]) for i, (a, b) in enumerate((
        (x_hbm.at[pl.ds(pl.multiple_of(v * 4 * OWN, 4 * OWN), 4 * OWN)], xh), (wq_hbm, wq), (wk_hbm, wk), (wv_hbm, wv)))]
    wo_load = local(wo_hbm, wo, loads.at[4])
    weights = [local(a, b, loads.at[5 + i]) for i, (a, b) in enumerate(((wg_hbm, wg), (wu_hbm, wu), (wd_hbm, wd)))]

    def cache_load(c):
        out = []
        for i, src in enumerate((kc_hbm, vc_hbm)):
            for q in range(4):
                first = pl.multiple_of(((v * 4 + q) * OWN + c * PART) * 32, PART * 32)
                out.append(local(src.at[pl.ds(first, PART * 32)],
                                 bank.at[pl.ds(cache_row + q * PART * 32, PART * 32), pl.ds(pl.multiple_of((2 * c + i) * 256, 256), 256)],
                                 caches.at[c, 4 * i + q]))
        return out

    for cp in early:
        cp.start()
    for cp in cache_load(0):
        cp.start()
    wo_load.start()
    for c in range(1, CHUNKS):
        for cp in cache_load(c):
            cp.start()
    for q in range(4):
        lens_s[OWN * q:OWN * q + OWN, :] = jnp.broadcast_to(lens[v * 4 + q], (OWN, OWN)).T
    meet_all(t, v)
    for cp in early:
        cp.wait()

    def rs_first(p, r, sems, c):
        return [send(p.at[h, rows(q, c)], r.at[h, slot, part(c)], sems, (c, 2 * h + slot), dev)
                for h, slot, q, dev in ((0, 1, tz, dev_x), (1, 1, tz, dev_y), (0, 0, tx, dev_x), (1, 0, ty, dev_y))]

    def rs_second(r, sems, c):
        return [send(fwd.at[h, part(c)], r.at[h, part(c)], sems, (c, h), dev) for h, dev in ((0, dev_y), (1, dev_x))]

    def rs_forward(p, r, r_next, sems, sems_next, c):
        first = rs_first(p, r, sems, c)
        for h, q, cp in ((0, ty, rs_second(r_next, sems_next, c)[0]), (1, tx, rs_second(r_next, sems_next, c)[1])):
            first[h].wait_recv()
            fwd[h, part(c)] = p[h, rows(q, c)] + r[h, 1, part(c)]
            cp.start()

    def rs_finish(p, r, r_next, sems, sems_next, c):
        first, second = rs_first(p, r, sems, c), rs_second(r_next, sems_next, c)
        out = []
        for h in range(2):
            first[2 + h].wait_recv()
            second[h].wait_recv()
            out.append(p[h, rows(t, c)] + r[h, 0, part(c)] + r_next[h, part(c)])
        for cp in first + second:
            cp.wait_send()
        return out

    def ag_first(c, sems):
        return [send(ag.at[h, rows(t, c)], ag.at[h, rows(t, c)], sems, (c, i), dev)
                for i, (h, dev) in enumerate(((0, dev_x), (1, dev_y), (1, dev_x), (0, dev_y)))]

    def ag_second(c, sems):
        return [send(ag.at[h, rows(q, c)], ag.at[h, rows(q, c)], sems, (c, h), dev) for h, q, dev in ((0, tx, dev_y), (1, ty, dev_x))]

    def each(body):
        lax.fori_loop(0, CHUNKS, lambda c, _: (body(c), 0)[1], 0)

    @each
    def _(c):
        for cp in cache_load(c):
            cp.wait()

        @pl.when(c == 0)
        def _():
            wo_load.wait()

        x = jnp.concatenate([xh[rows(q, c), :] for q in range(4)], axis=0)
        lens_c = jnp.concatenate([lens_s[rows(q, c), :1] for q in range(4)], axis=0)

        def cached(i):
            return lambda g: bank[pl.ds(cache_row + 256 * g, 256), pl.ds(pl.multiple_of((2 * c + i) * 256, 256), 256)]

        def put(j, res):
            h, first = j // 3, 384 * (j % 3)
            for q in range(4):
                p1[h, rows(q, c), first:first + 384] = res[PART * q:PART * q + PART]

        attend(x, lens_c, gains[0:1, :], freq[...], wq[...], wk[...], wv[...], wo, cached(0), cached(1), put)
        for cp in rs_first(p1, r1, s1, c):
            cp.start()

    for w in weights:
        w.start()

    @each
    def _(c):
        rs_forward(p1, r1, r2, s1, s2, c)

    @each
    def _(c):
        s_a, s_b = norm_halves(*rs_finish(p1, r1, r2, s1, s2, c), g_post)
        x_a = (xh[rows(t, c), :COLS].astype(F32) + s_a).astype(BF16)
        x_b = (xh[rows(t, c), COLS:].astype(F32) + s_b).astype(BF16)
        x1[part(c), :COLS] = x_a
        x1[part(c), COLS:] = x_b
        m_a, m_b = norm_halves(x_a.astype(F32), x_b.astype(F32), g_pre)
        ag[0, rows(t, c)] = m_a.astype(BF16).astype(F32)
        ag[1, rows(t, c)] = m_b.astype(BF16).astype(F32)
        for cp in ag_first(c, s3):
            cp.start()

    @each
    def _(c):
        for cp, nxt in zip(ag_first(c, s3)[:2], ag_second(c, s4)):
            cp.wait_recv()
            nxt.start()

    pl.semaphore_signal(free_sem, inc=1, device_id=(t, 1 - v), device_id_type=MESH)
    for w in weights:
        w.wait()

    @each
    def _(c):
        for cp in ag_first(c, s3)[2:] + ag_second(c, s4):
            cp.wait_recv()
        for cp in ag_first(c, s3) + ag_second(c, s4):
            cp.wait_send()
        for q in range(4):
            for h in range(2):
                mb[PART * q:PART * q + PART, COLS * h:COLS * h + COLS] = ag[h, rows(q, c)].astype(BF16)

        def up(j, _):
            cols = pl.ds(pl.multiple_of(j * 256, 256), 256)
            gate = jnp.dot(mb[...], wg[:, cols], preferred_element_type=F32)
            lift = jnp.dot(mb[...], wu[:, cols], preferred_element_type=F32)
            act[:, cols] = (jax.nn.gelu(gate, approximate=True) * lift).astype(BF16)
            return 0

        lax.fori_loop(0, d // 256, up, 0)
        for h in range(2):
            def down(j, _):
                res = jnp.dot(act[...], wd[:, pl.ds(pl.multiple_of(COLS * h + j * 384, 128), 384)], preferred_element_type=F32)
                for q in range(4):
                    p2[h, rows(q, c), pl.ds(pl.multiple_of(j * 384, 128), 384)] = res[PART * q:PART * q + PART]
                return 0

            lax.fori_loop(0, COLS // 384, down, 0)
        for cp in rs_first(p2, r1, s5, c):
            cp.start()

    me, oth = v * 4 + t, p1
    eb = bank.at[:SLOTS * TILE]
    yb = bank.at[SLOTS * TILE:SLOTS * TILE + 8 * OWN]
    tiles = e_hbm.shape[0] // TILE
    total = 2 * tiles

    def slot_of(g):
        return pl.ds(pl.multiple_of((g % SLOTS) * TILE, TILE), TILE)

    def fetch(g):
        src = e_hbm.at[pl.ds(pl.multiple_of((g % tiles) * TILE, TILE), TILE)]
        return local(src, eb.at[slot_of(g)], e_sem.at[g % SLOTS])

    for g in range(SLOTS):
        fetch(g).start()

    @each
    def _(c):
        rs_forward(p2, r1, r2, s5, s6, c)

    def cross_own(c):
        return send(ag.at[:, rows(t, c)], oth.at[:, rows(t, c)], s9, (c,), (t, 1 - v))

    pl.semaphore_wait(free_sem, 1)

    @each
    def _(c):
        s_a, s_b = norm_halves(*rs_finish(p2, r1, r2, s5, s6, c), g_mlp)
        ag[0, rows(t, c)] = (x1[part(c), :COLS].astype(F32) + s_a).astype(BF16).astype(F32)
        ag[1, rows(t, c)] = (x1[part(c), COLS:].astype(F32) + s_b).astype(BF16).astype(F32)
        cross_own(c).start()
        for cp in ag_first(c, s7):
            cp.start()

    block = lambda q: pl.ds(pl.multiple_of(q * OWN, OWN), OWN)
    cross = [send(ag.at[:, block(q)], oth.at[:, block(q)], s10, (i,), (t, 1 - v)) for i, q in enumerate((tx, ty, tz))]
    tot[...] = jnp.zeros_like(tot)
    hit[...] = jnp.zeros_like(hit)
    spots = [w * 4 + q for q in (t, tx, ty, tz) for w in (v, 1 - v)]
    for k, b in enumerate(spots):
        lane = tgt[b] - me * e_hbm.shape[0]
        dif[:, OWN * k:OWN * k + OWN] = lane - lax.broadcasted_iota(jnp.int32, (8, OWN), 0)

    def y_copy(b):
        return local(yb.at[block(b)], y_out.at[block(b)], y_sem.at[b])

    def prepare(src, w, q, ht, lanes):
        h_a, h_b = src[0, block(q)], src[1, block(q)]
        b = w * 4 + q
        yb[block(b), :COLS] = h_a.astype(BF16)
        yb[block(b), COLS:] = h_b.astype(BF16)
        y_copy(b).start()
        n_a, n_b = norm_halves(h_a, h_b, g_fin)
        ht[:COLS, lanes] = n_a.astype(BF16).T
        ht[COLS:, lanes] = n_b.astype(BF16).T

    prepare(ag, v, t, ht0, slice(0, OWN))

    @each
    def _(c):
        cross_own(c).wait_recv()

    prepare(oth, 1 - v, t, ht0, slice(OWN, 2 * OWN))

    def epilogue(lg, span, base, valid):
        s, k = head_epilogue(lg, dif[:, span], base)
        tot[:, span] += jnp.where(valid, s, 0.0)
        hit[:, span] += jnp.where(valid, k, 0.0)

    def body(i, offset, ht, bufs, span):
        g = i + offset
        fetch(g).wait()

        @pl.when((g >= 1) & (g + SLOTS - 1 < total))
        def _():
            fetch(g + SLOTS - 1).start()

        first = pl.multiple_of((g % SLOTS) * TILE, TILE)
        for k in range(TILE // SUB):
            cur, prev = bufs[k % 2], bufs[(k + 1) % 2]
            cur[...] = jnp.dot(bank[pl.ds(first + SUB * k, SUB), :], ht[...], preferred_element_type=F32)
            epilogue(prev[...], span, i * TILE + (k - 1) * SUB, True if k else i > 0)

    near, far = slice(0, 2 * OWN), slice(2 * OWN, 8 * OWN)
    near_bufs = (lg_a.at[:, near], lg_b.at[:, near])

    def pass_one(i, _):
        @pl.when((i >= 3) & (i < 15) & (i % 3 == 0))
        def _():
            c = i // 3 - 1
            for cp, nxt in zip(ag_first(c, s7)[:2], ag_second(c, s8)):
                cp.wait_recv()
                nxt.start()

        @pl.when(i == 16)
        def _():
            for c in range(CHUNKS):
                for cp in ag_first(c, s7)[2:]:
                    cp.wait_recv()
            cross[0].start()
            cross[1].start()

        @pl.when((i == 18) | (i == 20))
        def _():
            k = i - 18
            prepare(ag, v, tx + (k // 2) * (ty - tx), ht1, pl.ds(pl.multiple_of(k * OWN, OWN), OWN))

        @pl.when(i == 19)
        def _():
            cross[0].wait_recv()
            cross[1].wait_recv()

        @pl.when((i == 19) | (i == 21))
        def _():
            k = i - 18
            prepare(oth, 1 - v, tx + (k // 2) * (ty - tx), ht1, pl.ds(pl.multiple_of(k * OWN, OWN), OWN))

        @pl.when(i == 23)
        def _():
            for c in range(CHUNKS):
                for cp in ag_second(c, s8):
                    cp.wait_recv()
            cross[2].start()

        body(i, 0, ht0, near_bufs, near)
        return 0

    lax.fori_loop(0, tiles, pass_one, 0)
    epilogue(lg_b[:, near], near, tiles * TILE - SUB, True)
    prepare(ag, v, tz, ht1, slice(4 * OWN, 5 * OWN))
    cross[2].wait_recv()
    prepare(oth, 1 - v, tz, ht1, slice(5 * OWN, 6 * OWN))
    lax.fori_loop(0, tiles, lambda i, _: (body(i, tiles, ht1, (lg_a, lg_b), far), 0)[1], 0)
    epilogue(lg_b[...], far, tiles * TILE - SUB, True)

    for k, b in enumerate(spots):
        lanes = slice(OWN * k, OWN * k + OWN)
        sums[b, 0:1] = jnp.sum(tot[:, lanes], axis=0, keepdims=True)
        sums[b, 1:2] = jnp.sum(hit[:, lanes], axis=0, keepdims=True)
    outs = []
    for k in range(1, 8):
        dt, dv = k % 4, k // 4
        outs.append(send(sums, fin.at[k], s11, (k - 1,), ((t + dt) % 4, (v + dv) % 2)))
    for cp in outs:
        cp.start()
    acc = sums[...]
    for k in range(1, 8):
        outs[k - 1].wait_recv()
        acc += fin[k]
    lp_ref[...] = FINAL_CAP * acc[:, 1] - jnp.log(acc[:, 0])
    for c in range(CHUNKS):
        for cp in ag_first(c, s7) + ag_second(c, s8) + [cross_own(c)]:
            cp.wait_send()
    for cp in cross + outs:
        cp.wait_send()
    for b in range(8):
        y_copy(b).wait()


def step(x, lens, ga, gb, gc, gd, ge, freq, tgt, wq, wk, wv, wo, kc, vc, wg, wu, wd, table):
    d = x.shape[1]
    n = x.shape[0] // 2
    vm, hbm = pl.BlockSpec(memory_space=pltpu.VMEM), pl.BlockSpec(memory_space=pl.ANY)
    sem = lambda *k: pltpu.SemaphoreType.DMA(k)
    return pl.pallas_call(
        step_kernel,
        out_shape=[jax.ShapeDtypeStruct(x.shape, BF16), jax.ShapeDtypeStruct((8, OWN), F32)],
        in_specs=[hbm] + [vm] * 8 + [hbm] * 10,
        out_specs=[hbm, vm],
        scratch_shapes=[
            pltpu.VMEM((3 * d, d), BF16), pltpu.VMEM((n, d), BF16), pltpu.VMEM((OWN, d), BF16), pltpu.VMEM((2, n, COLS), F32),
            pltpu.VMEM((2, 2, OWN, COLS), F32), pltpu.VMEM((2, OWN, COLS), F32),
            pltpu.VMEM((2, OWN, COLS), F32), pltpu.VMEM((2, n, COLS), F32), pltpu.VMEM((2, n, COLS), F32),
            pltpu.VMEM((OWN, d), BF16), pltpu.VMEM((OWN, d), BF16), pltpu.VMEM((8, d), F32), pltpu.VMEM((n, 128), jnp.int32),
            pltpu.VMEM((d, 256), BF16), pltpu.VMEM((d, 768), BF16), pltpu.VMEM((SUB, 768), F32), pltpu.VMEM((SUB, 768), F32),
            pltpu.VMEM((8, 8 * OWN), jnp.int32), pltpu.VMEM((8, 8 * OWN), F32), pltpu.VMEM((8, 8 * OWN), F32),
            pltpu.VMEM((8, 2, OWN), F32), pltpu.VMEM((8, 8, 2, OWN), F32),
            sem(8), sem(CHUNKS, 8), sem(SLOTS), sem(8),
            sem(2, CHUNKS, 4), sem(2, CHUNKS, 2), sem(2, CHUNKS, 4), sem(2, CHUNKS, 2), sem(2, CHUNKS, 4), sem(2, CHUNKS, 2),
            sem(2, CHUNKS, 4), sem(2, CHUNKS, 2), sem(2, CHUNKS), sem(2, 3), sem(2, 7), pltpu.SemaphoreType.REGULAR],
        compiler_params=pltpu.CompilerParams(collective_id=0, has_side_effects=True, vmem_limit_bytes=VMEM_MAX),
        name='step',
    )(x, lens, ga, gb, gc, gd, ge, freq, tgt, wq, wk, wv, wo, kc, vc, wg, wu, wd, table)


def finish_kernel(y_hbm, lp_ref, y_out, lp_out, yb, sems):
    blocks = yb.shape[0]
    rows = yb.shape[1]
    take = [pltpu.make_async_copy(y_hbm.at[rows * i:rows * i + rows], yb.at[i], sems.at[0, i]) for i in range(blocks)]
    give = [pltpu.make_async_copy(yb.at[i], y_out.at[rows * i:rows * i + rows], sems.at[1, i]) for i in range(blocks)]
    for cp in take:
        cp.start()
    lp_out[...] = lp_ref[...]
    for a, b in zip(take, give):
        a.wait()
        b.start()
    for cp in give:
        cp.wait()


def finish(y, lp):
    vm, hbm = pl.BlockSpec(memory_space=pltpu.VMEM), pl.BlockSpec(memory_space=pl.ANY)
    return pl.pallas_call(
        finish_kernel,
        out_shape=[jax.ShapeDtypeStruct(y.shape, y.dtype), jax.ShapeDtypeStruct(lp.shape, lp.dtype)],
        in_specs=[hbm, vm],
        out_specs=[hbm, vm],
        scratch_shapes=[pltpu.VMEM((8, y.shape[0] // 8, y.shape[1]), y.dtype), pltpu.SemaphoreType.DMA((2, 8))],
        compiler_params=pltpu.CompilerParams(vmem_limit_bytes=VMEM_LIMIT),
        name='finish',
    )(y, lp)


def solution(mesh):
    in_specs = (P(), P(), P(), P(), P(None, 't'), P(None, 't'), P(None, 't'), P('t', None), P(), P(), P(None, 't'), P(None, 't'), P('t', None), P(), P(), P(None, None, 't', None), P(None, None, 't', None), P(('v', 't'), None))

    def local_step(hidden_in, seq_lens, target, g_attn_pre, w_q, w_k, w_v, w_o, g_attn_post, g_mlp_pre, w_gate, w_up, w_down, g_mlp_post, g_final, k_cache, v_cache, embed_table):
        freq = jnp.asarray((ROPE_BASE ** (-2.0 * np.arange(128, dtype=np.float32) / 256)).astype(np.float32)[None])
        hidden_out, logprob = step(hidden_in, seq_lens.reshape(8, 1, OWN), g_attn_pre, g_attn_post, g_mlp_pre, g_mlp_post, g_final, freq, target.reshape(8, 1, OWN), w_q, w_k, w_v, w_o,
                      k_cache.reshape(-1, 256), v_cache.reshape(-1, 256), w_gate, w_up, w_down, embed_table)
        hidden_out, logprob = finish(hidden_out, logprob)
        return logprob.reshape(-1), hidden_out

    return jax.shard_map(local_step, mesh=mesh, in_specs=in_specs, out_specs=(P(), P()), check_vma=False)
```
